256 devices in a mesh: grow: 8 (over y_hi, x), gcol: 32 (over y_lo, z, core).
Axes of the slice: x: 4, y: 4 (y_hi: 2, y_lo: 2; y = y_hi * 2 + y_lo), z: 8, core: 2. Of those that a mesh axis runs over, the one named last changes fastest.
Arguments:
- psi: float32 [262144, 1024], P(('grow', 'gcol')), may hold values from -6 to 6
- vpsi: float32 [262144, 1024], P(('grow', 'gcol')), may hold values from -24 to 24
- kinetic: float32 [262144], P(('grow', 'gcol')), may hold values from 0.1 to 10
- mixing: float32 [1024, 1024], P('grow', 'gcol'), may hold values from -0.1875 to 0.1875
Outputs:
- residual: float32 [262144, 1024], P(('grow', 'gcol'))
- projected: float32 [1024, 1024], P('grow', 'gcol')
The draws below stay inside these ranges and needn't reach their ends.
All inputs are finite; a program needn't handle non-finite values.
Results may differ from the reference program's by a relative error of at most 0.000073.
Values sent between devices are 32-bit elements; how exact they have to be, the bound alone decides.
A program may use at most 128 MiB of HBM per device.

```python
import math
import jax
import jax.numpy as jnp
from jax import lax

NB = 1024
ROWS = 262144


def spiked(result, rng, source, target, blocks, factor):
    owner, partner = [(jnp.arange(result.shape[position]) // (result.shape[position] // blocks)).reshape([-1 if axis == position else 1 for axis in range(result.ndim)]) for position in (source, target)]
    chosen = jax.random.permutation(rng, blocks)[partner]
    strong = (owner == chosen) | (owner == (partner + blocks // 2) % blocks)
    return jnp.where(strong, factor * result, result)


def steps_of(stream_key, shape, split, least, high):
    factor_of = 1.0
    for position, blocks in split:
        steps = jax.random.uniform(jax.random.fold_in(jax.random.fold_in(stream_key, 6), position), (blocks,), jnp.float32, least / len(split), high / len(split))
        factor_of = factor_of * jnp.repeat(jnp.exp(steps), shape[position] // blocks).reshape((-1,) + (1,) * (len(shape) - 1 - position))
    return factor_of


def normal_values(key, shape, spread, reach, shards=(), dtype=jnp.bfloat16):
    values = jax.random.normal(key, shape, jnp.float32) * spread
    if len(shards) > 0:
        values = steps_of(key, shape, shards, -0.22, 0.18) * values
    return jnp.clip(values, min=-reach, max=reach).astype(dtype)


def heavy_noise(own_key, dims, spread, reach, shards, heavy, held_as=jnp.bfloat16):
    values = spread * jax.random.normal(own_key, dims, jnp.float32)
    if shards:
        values = values * steps_of(own_key, dims, shards, -0.22, 0.18)
    return jnp.clip(spiked(values, jax.random.fold_in(own_key, 3), *heavy), -reach, reach).astype(held_as)


def setup_inputs(seed: int = 0) -> dict:
    keys = jax.random.split(jax.random.key(seed), 5)
    psi = normal_values(keys[0], (ROWS, NB), 1.0, 6.0, ((0, 256),), jnp.float32)
    vpsi = heavy_noise(keys[1], (ROWS, NB), 1.0, 24.0, ((0, 256),), (0, 1, 256, 6.0), jnp.float32)
    kinetic = jnp.clip(jnp.exp(math.log(10.0) - 4.6051702 * jax.random.uniform(keys[2], (ROWS,), jnp.float32) ** steps_of(keys[2], (ROWS,), ((0, 256),), -0.2, 0.2)), 0.1, 10.0)
    mixing = normal_values(keys[3], (NB, NB), NB ** -0.5, 0.1875, ((0, 8), (1, 32)), jnp.float32)
    return dict(psi=psi, vpsi=vpsi, kinetic=kinetic, mixing=mixing)


def reference(psi, vpsi, kinetic, mixing):
    hpsi = kinetic[:, None] * psi + vpsi
    projected = lax.dot_general(psi, hpsi, (((0,), (0,)), ((), ())), precision=lax.Precision.HIGHEST, preferred_element_type=jnp.float32) * (1.0 / ROWS)
    correction = hpsi - jnp.dot(psi, projected, precision=lax.Precision.HIGHEST, preferred_element_type=jnp.float32)
    residual = jnp.dot(correction, mixing, precision=lax.Precision.HIGHEST, preferred_element_type=jnp.float32)
    return residual, projected
```

```python
import jax
import jax.numpy as jnp
from jax import lax
from jax.experimental import pallas as pl
from jax.experimental.pallas import tpu as pltpu
from jax.sharding import PartitionSpec as P

MESH = pl.DeviceIdType.MESH
F32, BF16 = jnp.float32, jnp.bfloat16
N_COPIES = 224


def split(value):
    high = value.astype(BF16)
    return high, (value - high.astype(F32)).astype(BF16)


def dot(a, b):
    return lax.dot_general(a, b, (((1,), (0,)), ((), ())), preferred_element_type=F32)


def dot3(a_high, a_low, b_high, b_low):
    return dot(a_high, b_high) + dot(a_high, b_low) + dot(a_low, b_high)


def mod(a, n):
    return lax.rem(a, n)


def aligned(start, size, unit):
    return pl.ds(pl.multiple_of(start, unit), size)


def kernel(
    psi_hbm, vpsi_hbm, kin_hbm, mix_hbm, acc, proj_hbm,
    psi_v, kin_v, kin_cols, psi_h, psi_l, pt_h, pt_l, h_h, h_l,
    pb, pr, relay, xr, own, yr, zs, zr, pg, po, mg, m_h, m_l, qa, qb, proj_v,
    load_sem, out_sem, send_sem, recv_sem,
):
    row, col = lax.axis_index("grow"), lax.axis_index("gcol")
    x, y_hi = mod(row, 4), lax.div(row, 4)
    core, z, y_lo = mod(col, 2), mod(lax.div(col, 2), 8), lax.div(col, 16)
    y = 2 * y_hi + y_lo
    other_core = 1 - core
    z_odd = mod(z, 2)

    def at(x=x, y=y, z=z, core=core):
        return (4 * lax.div(y, 2) + x, (mod(y, 2) * 8 + z) * 2 + core)

    sent = []

    def send(src, dst, to):
        i = len(sent)
        copy = pltpu.make_async_remote_copy(
            src_ref=src, dst_ref=dst, send_sem=send_sem.at[i], recv_sem=recv_sem.at[i], device_id=to, device_id_type=MESH
        )
        copy.start()
        sent.append(copy)
        return copy

    own_mix = mg.at[core, z, y_hi, 4 * y_lo + x]
    small = [pltpu.make_async_copy(kin_hbm, kin_v, out_sem.at[0]), pltpu.make_async_copy(mix_hbm, own_mix, out_sem.at[1])]
    for copy in small:
        copy.start()
    for i in range(8):
        rows = pl.ds(128 * i, 128)
        pltpu.make_async_copy(psi_hbm.at[rows], psi_v.at[rows], load_sem.at[0, i]).start()
        pltpu.make_async_copy(vpsi_hbm.at[rows], acc.at[rows], load_sem.at[1, i]).start()

    flip_y = y + 1 - 2 * y_lo
    partner = at(core=other_core)
    plane = [at(x=mod(x + dx, 4), y=mod(y + dy, 4)) for dx in range(4) for dy in range(4) if dx + dy > 0]
    peers = [partner, at(y=flip_y, core=other_core)] + plane + [at(z=mod(z + d, 8)) for d in range(1, 8)]
    barrier = pltpu.get_barrier_semaphore()
    for peer in peers:
        pl.semaphore_signal(barrier, inc=1, device_id=peer, device_id_type=MESH)

    for copy in small:
        copy.wait()
    turned = jnp.transpose(jnp.concatenate([kin_v[...]] * 16, axis=0))
    for i in range(8):
        kin_cols[i] = jnp.broadcast_to(turned[:, i : i + 1], (128, 128))

    def prepare(i, carry):
        rows = aligned(128 * i, 128, 128)
        pltpu.make_async_copy(psi_hbm.at[rows], psi_v.at[rows], load_sem.at[0, i]).wait()
        pltpu.make_async_copy(vpsi_hbm.at[rows], acc.at[rows], load_sem.at[1, i]).wait()
        kin = kin_cols[i]
        for j in range(8):
            cols = pl.ds(128 * j, 128)
            tile = psi_v[rows, cols]
            high, low = split(kin * tile + acc[rows, cols])
            h_h[rows, cols] = high
            h_l[rows, cols] = low
            high, low = split(jnp.transpose(tile))
            pt_h[cols, rows] = high
            pt_l[cols, rows] = low
        return carry

    lax.fori_loop(0, 8, prepare, 0)

    pl.semaphore_wait(barrier, len(peers))

    spread = [send(own_mix, own_mix, peer) for peer in plane]

    shared = []

    def mixing_pass(slab, half):
        ref = mg.at[core, slab, half]
        shared.append(send(ref, ref, partner))

    def mixing_send(slab, half, step):
        ref = mg.at[core, slab, half]
        return send(ref, ref, at(z=mod(z + step + 8, 8)))

    up, down = {}, {}

    def mixing_start():
        for copy in spread:
            copy.wait_recv()
        up[1, 0] = mixing_send(z, 0, 1)
        down[1, 0] = mixing_send(z, 1, -1)
        up[1, 1] = mixing_send(z, 1, 1)
        down[1, 1] = mixing_send(z, 0, -1)
        for half in range(2):
            mixing_pass(z, half)

    def mixing_step(distance, k):
        below, above = mod(z + 8 - distance, 8), mod(z + distance, 8)
        more = distance < 3 or (distance == 3 and k == 0)
        up[distance, k].wait_recv()
        if more:
            up[distance + 1, k] = mixing_send(below, k, 1)
        mixing_pass(below, k)
        down[distance, k].wait_recv()
        if more:
            down[distance + 1, k] = mixing_send(above, 1 - k, -1)
        mixing_pass(above, 1 - k)

    first, second = (x, y), (y, x)

    def to_first(part, f):
        return at(x=f) if part == 0 else at(y=f)

    def to_second(part, s):
        return at(y=s) if part == 0 else at(x=s)

    def share(part, off):
        target = mod(first[part] + off, 4)
        pieces = []
        for half in range(2):
            for s in range(4):
                tx, ty = (target, s) if part == 0 else (s, target)
                start = 512 * lax.div(ty, 2) + 128 * tx + 64 * mod(ty, 2) + 32 * half
                pieces.append(aligned(start, 32, 32))
        lhs_h = jnp.concatenate([pt_h[p, :] for p in pieces], axis=0)
        lhs_l = jnp.concatenate([pt_l[p, :] for p in pieces], axis=0)
        for n in range(2):
            cols = pl.ds(512 * part + 256 * n, 256)
            out = dot3(lhs_h, lhs_l, h_h[:, cols], h_l[:, cols])
            pb[part, off, 0, :, pl.ds(256 * n, 256)] = out[:128]
            pb[part, off, 1, :, pl.ds(256 * n, 256)] = out[128:]
        return send(pb.at[part, off, other_core], pr.at[part, off], partner)

    def joined(part, off, copy):
        copy.wait_recv()
        pb[part, off, core] += pr[part, off]

    late, early = pl.ds(0, 64), pl.ds(64, 64)
    relays, direct = {}, {}

    def far(part, copy):
        joined(part, 2, copy)
        f = first[part]
        block = pb.at[part, 2, core]
        relays[part] = (
            send(block.at[late], relay.at[part, 0], to_first(part, mod(f + 1, 4))),
            send(block.at[early], relay.at[part, 1], to_first(part, mod(f + 3, 4))),
        )

    def near(part, off, copy):
        joined(part, off, copy)
        side, rows = (0, early) if off == 1 else (1, late)
        block = pb.at[part, off, core]
        direct[part, off] = [send(block.at[rows], xr.at[part, side, rows], to_first(part, mod(first[part] + off, 4)))]

    def relayed(part, off):
        side, rows = (0, late) if off == 1 else (1, early)
        relays[part][side].wait_recv()
        pb[part, off, core, rows] += relay[part, side]
        block = pb.at[part, off, core]
        direct[part, off].append(send(block.at[rows], xr.at[part, side, rows], to_first(part, mod(first[part] + off, 4))))

    seconds = {}

    def own_first(part):
        for off in (1, 3):
            for copy in direct[part, off]:
                copy.wait_recv()
        own[part] = (pb[part, 0, core] + xr[part, 0] + xr[part, 1]).reshape(4, 32, 512)
        s = second[part]
        seconds[part] = [
            send(own.at[part, mod(s + d, 4)], yr.at[part, d - 1], to_second(part, mod(s + d, 4))) for d in (2, 1, 3)
        ]

    def own_second(part):
        for copy in seconds[part]:
            copy.wait_recv()
        total = own[part, second[part]] + yr[part, 0] + yr[part, 1] + yr[part, 2]
        for j in range(4):
            zs[4 * part + j] = total[:, 128 * j : 128 * (j + 1)]

    a2 = share(0, 2)
    b2 = share(1, 2)
    far(0, a2)
    a1 = share(0, 1)
    far(1, b2)
    b1 = share(1, 1)
    near(0, 1, a1)
    a3 = share(0, 3)
    near(1, 1, b1)
    b3 = share(1, 3)
    near(0, 3, a3)
    mixing_start()
    a0 = share(0, 0)
    near(1, 3, b3)
    relayed(0, 1)
    relayed(0, 3)
    b0 = share(1, 0)
    relayed(1, 1)
    relayed(1, 3)
    joined(0, 0, a0)
    joined(1, 0, b0)

    def natural(i, carry):
        rows = aligned(128 * i, 128, 128)
        high, low = split(psi_v[rows, :])
        psi_h[rows, :] = high
        psi_l[rows, :] = low
        return carry

    lax.fori_loop(0, 8, natural, 0)
    mixing_step(1, 0)
    own_first(0)
    own_first(1)
    mixing_step(1, 1)
    own_second(0)
    own_second(1)
    order = (4, 3, 5, 2, 6, 1, 7)
    z_copies = []
    for d in order:
        to = mod(z + d, 8)
        z_copies.append(send(zs.at[to], zr.at[d - 1], at(z=to)))
    mixing_step(2, 0)
    mixing_step(2, 1)
    for copy in z_copies:
        copy.wait_recv()
    total = zs[z]
    for d in range(7):
        total = total + zr[d]
    pg[z] = total * (1.0 / (256 * 1024))
    z_copies = [send(pg.at[z], pg.at[z], at(z=mod(z + d, 8))) for d in order]
    mixing_step(3, 0)
    mixing_step(3, 1)
    mixing_step(4, 0)
    for copy in shared:
        copy.wait_recv()

    def mixing_split(i, carry):
        for half in range(2):
            for k in range(8):
                tile = jnp.concatenate([mg[c, 2 * i + odd, half, k] for odd in range(2) for c in range(2)], axis=0)
                where = (pl.ds(512 * half + 128 * (k % 4), 128), aligned(512 * (k // 4) + 128 * i, 128, 128))
                high, low = split(jnp.transpose(tile))
                m_h[where] = high
                m_l[where] = low
        return carry

    lax.fori_loop(0, 4, mixing_split, 0)

    for copy in z_copies:
        copy.wait_recv()

    block = 4 * y_lo + lax.div(z, 2)
    group = 2 * y_lo + core
    po[group] = pg[block]
    out_copies = []
    for dy, dc in ((0, 1), (1, 0), (1, 1)):
        to_y, to_core = (flip_y if dy else y), (other_core if dc else core)
        out_copies.append(send(pg.at[4 * mod(to_y, 2) + lax.div(z, 2)], po.at[group], at(y=to_y, core=to_core)))

    p_h, p_l = split(jnp.concatenate([pg[j] for j in range(8)], axis=1))
    for n in range(4):
        cols = pl.ds(256 * n, 256)
        value = -dot3(p_h, p_l, m_h[:, cols], m_l[:, cols])
        if n < 2:
            qa[core, x, y, :, pl.ds(256 * n, 256)] = value
        else:
            qb[core, y, x, :, pl.ds(256 * n - 512, 256)] = value
    q = (qa, qb)
    ones, ups, downs, across = {}, {}, {}, {}

    def piece(part, off, r):
        return q[part].at[core, mod(first[part] + off, 4), mod(second[part] + r, 4)]

    def q_up(part, off, r):
        ref = piece(part, off, r)
        ups[part, off, r] = send(ref, ref, to_first(part, mod(first[part] + 1, 4)))

    def q_down(part, off, r):
        ref = piece(part, off, r)
        downs[part, off, r] = send(ref, ref, to_first(part, mod(first[part] + 3, 4)))

    def q_pass(part, off, r):
        ref = piece(part, off, r)
        across[part, off, r] = send(ref, ref, partner)

    def q_spread(part):
        ref = piece(part, 0, 0)
        for d in (2, 1, 3):
            ones[part, d] = send(ref, ref, to_second(part, mod(second[part] + d, 4)))
        q_up(part, 0, 0)
        q_down(part, 0, 0)
        q_pass(part, 0, 0)

    def q_second(part):
        ones[part, 3].wait_recv()
        q_up(part, 0, 1)
        ones[part, 1].wait_recv()
        q_down(part, 0, 3)
        q_up(part, 0, 3)
        ones[part, 2].wait_recv()
        q_down(part, 0, 2)
        q_up(part, 0, 2)
        q_down(part, 0, 1)
        for r in (1, 2, 3):
            q_pass(part, 0, r)

    def q_from_below(part, r):
        ups[part, 0, r].wait_recv()
        if r < 2:
            q_up(part, 3, r)
        q_pass(part, 3, r)

    def q_from_above(part, r):
        downs[part, 0, r].wait_recv()
        if r >= 2:
            q_down(part, 1, r)
        q_pass(part, 1, r)

    def q_opposite(part):
        for r in range(4):
            (ups[part, 3, r] if r < 2 else downs[part, 1, r]).wait_recv()
            q_pass(part, 2, r)

    def q_here(part, off):
        for r in range(4):
            across[part, off, r].wait_recv()

    def product(i, carry):
        rows = aligned(512 * mod(i, 2), 512, 512)
        cols = aligned(256 * lax.div(i, 2), 256, 256)
        acc[rows, cols] = dot3(h_h[rows, :], h_l[rows, :], m_h[:, cols], m_l[:, cols])
        return carry

    q_spread(0)
    q_spread(1)
    lax.fori_loop(0, 4, product, 0)
    q_second(0)
    q_second(1)
    for part in range(2):
        q_from_below(part, 0)
        q_from_above(part, 0)
    lax.fori_loop(4, 8, product, 0)

    def final_x(target):
        rhs_h, rhs_l = split(
            jnp.concatenate([qa[c, target, yy] for yy in range(4) for c in range(2)], axis=0)
        )
        k0, k1 = aligned(128 * target, 128, 128), aligned(512 + 128 * target, 128, 128)

        def rows_of(i, carry):
            rows = aligned(256 * i, 256, 256)
            lhs_h = jnp.concatenate([psi_h[rows, k0], psi_h[rows, k1]], axis=1)
            lhs_l = jnp.concatenate([psi_l[rows, k0], psi_l[rows, k1]], axis=1)
            acc[rows, :512] += dot3(lhs_h, lhs_l, rhs_h, rhs_l)
            return carry

        for i in range(4):
            rows_of(i, 0)

    def final_y(target):
        rhs_h, rhs_l = split(
            jnp.concatenate([qb[c, 2 * target + yl, xx] for xx in range(4) for yl in range(2) for c in range(2)], axis=0)
        )
        k = aligned(512 * target, 512, 512)
        for i in range(4):
            rows = pl.ds(256 * i, 256)
            acc[rows, 512:] += dot3(psi_h[rows, k], psi_l[rows, k], rhs_h, rhs_l)

    for part in range(2):
        q_from_below(part, 1)
        q_from_above(part, 3)
    q_here(0, 0)
    final_x(x)
    for part in range(2):
        q_from_above(part, 2)
        q_from_below(part, 3)
        q_from_below(part, 2)
        q_from_above(part, 1)
    q_here(0, 3)
    final_x(mod(x + 3, 4))
    q_here(0, 1)
    final_x(mod(x + 1, 4))
    for off in (0, 1, 3):
        q_here(1, off)
    final_y(y_hi)
    for copy in out_copies:
        copy.wait_recv()
    proj_v[...] = jnp.transpose(jnp.concatenate([po[j] for j in range(4)], axis=0))
    mine = aligned(32 * (2 * z_odd + core), 32, 32)
    out = pltpu.make_async_copy(proj_v.at[mine], proj_hbm, out_sem.at[0])
    out.start()
    q_opposite(0)
    q_opposite(1)
    q_here(0, 2)
    final_x(mod(x + 2, 4))
    q_here(1, 2)
    final_y(1 - y_hi)
    for copy in sent:
        copy.wait_send()
    out.wait()


def body(psi, vpsi, kinetic, mixing):
    anywhere = pl.BlockSpec(memory_space=pl.ANY)
    shapes = [
        ((1024, 1024), F32), ((8, 128), F32), ((8, 128, 128), F32),
        ((1024, 1024), BF16), ((1024, 1024), BF16), ((1024, 1024), BF16), ((1024, 1024), BF16), ((1024, 1024), BF16), ((1024, 1024), BF16),
        ((2, 4, 2, 128, 512), F32), ((2, 4, 128, 512), F32), ((2, 2, 64, 512), F32), ((2, 2, 128, 512), F32), ((2, 4, 32, 512), F32),
        ((2, 3, 32, 512), F32), ((8, 32, 128), F32), ((7, 32, 128), F32), ((8, 32, 128), F32), ((4, 32, 128), F32),
        ((2, 8, 2, 8, 32, 128), F32), ((1024, 1024), BF16), ((1024, 1024), BF16),
        ((2, 4, 4, 32, 512), F32), ((2, 4, 4, 32, 512), F32), ((128, 128), F32),
    ]
    residual, projected = pl.pallas_call(
        kernel,
        out_shape=(
            pltpu.VMEM((1024, 1024), F32),
            jax.ShapeDtypeStruct((32, 128), F32),
        ),
        in_specs=[anywhere] * 4,
        out_specs=(pl.BlockSpec(memory_space=pltpu.VMEM), anywhere),
        scratch_shapes=[pltpu.VMEM(shape, dtype) for shape, dtype in shapes]
        + [
            pltpu.SemaphoreType.DMA((2, 8)),
            pltpu.SemaphoreType.DMA((3,)),
            pltpu.SemaphoreType.DMA((N_COPIES,)),
            pltpu.SemaphoreType.DMA((N_COPIES,)),
        ],
        compiler_params=pltpu.CompilerParams(
            collective_id=0, has_side_effects=True, vmem_limit_bytes=56 * 1024 * 1024
        ),
    )(psi, vpsi, kinetic.reshape(8, 128), mixing.T)
    return residual, projected.T


def solution(mesh):
    placed = (P(("grow", "gcol"), None), P(("grow", "gcol"), None), P(("grow", "gcol")), P("grow", "gcol"))
    return jax.shard_map(
        body,
        mesh=mesh,
        in_specs=placed,
        out_specs=(P(("grow", "gcol"), None), P("grow", "gcol")),
        check_vma=False,
    )
```

```python
import jax
import jax.numpy as jnp
from jax import lax
from jax.experimental import pallas as pl
from jax.experimental.pallas import tpu as pltpu
from jax.sharding import PartitionSpec as P

MESH = pl.DeviceIdType.MESH
F32, BF16 = jnp.float32, jnp.bfloat16
FAMILIES = ("spread", "share", "relay", "direct", "second", "mix", "pass", "zsum", "zall", "out", "ones", "turn", "across")
SLOTS = 80


def split(value):
    high = value.astype(BF16)
    return high, (value - high.astype(F32)).astype(BF16)


def dot(a, b):
    return lax.dot_general(a, b, (((1,), (0,)), ((), ())), preferred_element_type=F32)


def dot3(a_high, a_low, b_high, b_low):
    return dot(a_high, b_high) + dot(a_high, b_low) + dot(a_low, b_high)


def mod(a, n):
    return lax.rem(a, n)


def aligned(start, size, unit):
    return pl.ds(pl.multiple_of(start, unit), size)


def kernel(
    psi_hbm, vpsi_hbm, kin_hbm, mix_hbm, acc, proj_hbm,
    psi_v, kin_v, kin_cols, psi_h, psi_l, turn_h, turn_l, pt_h, pt_l, h_h, h_l,
    pb, pr, relay, xr, own, yr, zs, zr, pg, po, mg, m_h, m_l, qa, qb, q_own, proj_v,
    load_sem, out_sem, send_sem, recv_sem,
):
    row, col = lax.axis_index("grow"), lax.axis_index("gcol")
    x, y_hi = mod(row, 4), lax.div(row, 4)
    core, z, y_lo = mod(col, 2), mod(lax.div(col, 2), 8), lax.div(col, 16)
    y = 2 * y_hi + y_lo
    other_core = 1 - core
    z_odd = mod(z, 2)

    def at(x=x, y=y, z=z, core=core):
        return (4 * lax.div(y, 2) + x, (mod(y, 2) * 8 + z) * 2 + core)

    slots = iter(range(SLOTS))

    def send(family, src, dst, to, slot=None):
        copy = pltpu.make_async_remote_copy(
            src_ref=src,
            dst_ref=dst,
            send_sem=send_sem.at[FAMILIES.index(family)],
            recv_sem=recv_sem.at[next(slots) if slot is None else slot],
            device_id=to,
            device_id_type=MESH,
        )
        copy.start()
        return copy

    def wait_bytes(ref, sem):
        pltpu.make_async_copy(ref, ref, sem).wait()

    def arrived(ref, slot):
        wait_bytes(ref, recv_sem.at[slot])

    own_mix = mg.at[core, z, y_hi, 4 * y_lo + x]
    small = [pltpu.make_async_copy(kin_hbm, kin_v, out_sem.at[0]), pltpu.make_async_copy(mix_hbm, own_mix, out_sem.at[1])]
    for copy in small:
        copy.start()
    for i in range(8):
        rows = pl.ds(128 * i, 128)
        pltpu.make_async_copy(psi_hbm.at[rows], psi_v.at[rows], load_sem.at[i]).start()
        pltpu.make_async_copy(vpsi_hbm.at[rows], acc.at[rows], load_sem.at[i]).start()

    flip_y = y + 1 - 2 * y_lo
    partner = at(core=other_core)
    plane = [at(x=mod(x + dx, 4), y=mod(y + dy, 4)) for dx in range(4) for dy in range(4) if dx + dy > 0]
    peers = [partner, at(y=flip_y, core=other_core)] + plane + [at(z=mod(z + d, 8)) for d in range(1, 8)]
    barrier = pltpu.get_barrier_semaphore()
    for peer in peers:
        pl.semaphore_signal(barrier, inc=1, device_id=peer, device_id_type=MESH)

    for copy in small:
        copy.wait()
    turned = jnp.transpose(jnp.concatenate([kin_v[...]] * 16, axis=0))
    for i in range(8):
        kin_cols[i] = jnp.broadcast_to(turned[:, i : i + 1], (128, 128))

    def prepare(i, carry):
        rows = aligned(128 * i, 128, 128)
        wait_bytes(psi_v.at[pl.ds(0, 256)], load_sem.at[i])
        kin = kin_cols[i]
        for j in range(8):
            cols = pl.ds(128 * j, 128)
            tile = psi_v[rows, cols]
            high, low = split(kin * tile + acc[rows, cols])
            h_h[rows, cols] = high
            h_l[rows, cols] = low
            high, low = split(jnp.transpose(tile))
            pt_h[cols, rows] = high
            pt_l[cols, rows] = low
        return carry

    lax.fori_loop(0, 8, prepare, 0)

    pl.semaphore_wait(barrier, len(peers))

    plane_blocks = pr.at[0, 0, pl.ds(0, 120)]
    spread = next(slots)
    for peer in plane:
        send("spread", own_mix, own_mix, peer, spread)

    passed = [next(slots) for distance in range(5)]

    def mixing_pass(slab, half, distance):
        ref = mg.at[core, slab, half]
        send("pass", ref, ref, partner, passed[distance])

    def mixing_here(distance):
        arrived(mg.at[0, 0] if distance in (0, 4) else mg.at[0, pl.ds(0, 2)], passed[distance])

    def mixing_send(slab, half, step):
        ref = mg.at[core, slab, half]
        return send("mix", ref, ref, at(z=mod(z + step + 8, 8)))

    up, down = {}, {}

    def mixing_start():
        arrived(plane_blocks, spread)
        up[1, 0] = mixing_send(z, 0, 1)
        down[1, 0] = mixing_send(z, 1, -1)
        up[1, 1] = mixing_send(z, 1, 1)
        down[1, 1] = mixing_send(z, 0, -1)
        for half in range(2):
            mixing_pass(z, half, 0)

    def mixing_step(distance, k):
        below, above = mod(z + 8 - distance, 8), mod(z + distance, 8)
        more = distance < 3 or (distance == 3 and k == 0)
        up[distance, k].wait_recv()
        if more:
            up[distance + 1, k] = mixing_send(below, k, 1)
        mixing_pass(below, k, distance)
        down[distance, k].wait_recv()
        if more:
            down[distance + 1, k] = mixing_send(above, 1 - k, -1)
        mixing_pass(above, 1 - k, distance)

    z_pair = lax.div(z, 2)
    pairs = (z_pair, mod(z_pair + 3 + 2 * z_odd, 4), mod(z_pair + 5 - 2 * z_odd, 4), mod(z_pair + 2, 4))

    def mixing_split(pair):
        for half in range(2):
            for k in range(8):
                tile = jnp.concatenate([mg[c, 2 * pair + odd, half, k] for odd in range(2) for c in range(2)], axis=0)
                where = (pl.ds(512 * half + 128 * (k % 4), 128), aligned(256 * pair + 128 * (k // 4), 128, 128))
                high, low = split(jnp.transpose(tile))
                m_h[where] = high
                m_l[where] = low

    def product(pair):
        cols = aligned(256 * pair, 256, 256)

        def rows_of(i, carry):
            rows = aligned(512 * i, 512, 512)
            psi_v[rows, cols] = dot3(h_h[rows, :], h_l[rows, :], m_h[:, cols], m_l[:, cols])
            return carry

        lax.fori_loop(0, 2, rows_of, 0)

    first, second = (x, y), (y, x)

    def to_first(part, f):
        return at(x=f) if part == 0 else at(y=f)

    def to_second(part, s):
        return at(y=s) if part == 0 else at(x=s)

    def share(part, off):
        target = mod(first[part] + off, 4)
        pieces = []
        for half in range(2):
            for s in range(4):
                tx, ty = (target, s) if part == 0 else (s, target)
                start = 512 * lax.div(ty, 2) + 128 * tx + 64 * mod(ty, 2) + 32 * half
                pieces.append(aligned(start, 32, 32))
        lhs_h = jnp.concatenate([pt_h[p, :] for p in pieces], axis=0)
        lhs_l = jnp.concatenate([pt_l[p, :] for p in pieces], axis=0)
        for n in range(2):
            cols = pl.ds(512 * part + 256 * n, 256)
            out = dot3(lhs_h, lhs_l, h_h[:, cols], h_l[:, cols])
            pb[part, off, 0, :, pl.ds(256 * n, 256)] = out[:128]
            pb[part, off, 1, :, pl.ds(256 * n, 256)] = out[128:]
        return send("share", pb.at[part, off, other_core], pr.at[part, off], partner)

    def joined(part, off, copy):
        copy.wait_recv()
        pb[part, off, core] += pr[part, off]

    late, early = pl.ds(0, 64), pl.ds(64, 64)
    relays, direct = {}, {}

    def far(part, copy):
        joined(part, 2, copy)
        f = first[part]
        block = pb.at[part, 2, core]
        relays[part] = (
            send("relay", block.at[late], relay.at[part, 0], to_first(part, mod(f + 1, 4))),
            send("relay", block.at[early], relay.at[part, 1], to_first(part, mod(f + 3, 4))),
        )

    def near(part, off, copy):
        joined(part, off, copy)
        side, rows = (0, early) if off == 1 else (1, late)
        block = pb.at[part, off, core]
        direct[part, off] = next(slots)
        send("direct", block.at[rows], xr.at[part, side, rows], to_first(part, mod(first[part] + off, 4)), direct[part, off])

    def relayed(part, off):
        side, rows = (0, late) if off == 1 else (1, early)
        relays[part][side].wait_recv()
        pb[part, off, core, rows] += relay[part, side]
        block = pb.at[part, off, core]
        send("direct", block.at[rows], xr.at[part, side, rows], to_first(part, mod(first[part] + off, 4)), direct[part, off])

    seconds = {}

    def own_first(part):
        arrived(xr.at[part, 0], direct[part, 1])
        arrived(xr.at[part, 1], direct[part, 3])
        own[part] = (pb[part, 0, core] + xr[part, 0] + xr[part, 1]).reshape(4, 32, 512)
        s = second[part]
        seconds[part] = next(slots)
        for d in (2, 1, 3):
            to = mod(s + d, 4)
            send("second", own.at[part, to], yr.at[part, d - 1], to_second(part, to), seconds[part])

    def own_second(part):
        arrived(yr.at[part], seconds[part])
        total = own[part, second[part]] + yr[part, 0] + yr[part, 1] + yr[part, 2]
        for j in range(4):
            zs[4 * part + j] = total[:, 128 * j : 128 * (j + 1)]

    a2 = share(0, 2)
    b2 = share(1, 2)
    far(0, a2)
    a1 = share(0, 1)
    far(1, b2)
    b1 = share(1, 1)
    near(0, 1, a1)
    a3 = share(0, 3)
    near(1, 1, b1)
    mixing_start()
    b3 = share(1, 3)
    near(0, 3, a3)
    a0 = share(0, 0)
    near(1, 3, b3)
    relayed(0, 1)
    relayed(0, 3)
    b0 = share(1, 0)
    relayed(1, 1)
    relayed(1, 3)
    joined(0, 0, a0)
    joined(1, 0, b0)
    mixing_step(1, 0)
    def natural(i, carry):
        rows = aligned(128 * i, 128, 128)
        high, low = split(psi_v[rows, :])
        psi_h[rows, :] = high
        psi_l[rows, :] = low
        for k in range(4):
            left, right = psi_v[rows, 256 * k : 256 * k + 128], psi_v[rows, 256 * k + 128 : 256 * (k + 1)]
            for yl in range(2):
                lanes = slice(64 * yl, 64 * (yl + 1))
                high, low = split(jnp.concatenate([left[:, lanes], right[:, lanes]], axis=1))
                cols = pl.ds(512 * (k // 2) + 256 * yl + 128 * (k % 2), 128)
                turn_h[rows, cols] = high
                turn_l[rows, cols] = low
        return carry

    lax.fori_loop(0, 8, natural, 0)
    own_first(0)
    own_first(1)
    mixing_step(1, 1)

    mixing_here(0)
    mixing_here(1)
    mixing_split(pairs[0])
    mixing_step(2, 0)
    product(pairs[0])
    own_second(0)
    own_second(1)
    order = (4, 3, 5, 2, 6, 1, 7)
    z_sum, z_all = next(slots), next(slots)
    for d in order:
        to = mod(z + d, 8)
        send("zsum", zs.at[to], zr.at[d - 1], at(z=to), z_sum)
    mixing_step(2, 1)
    mixing_here(2)
    mixing_split(pairs[1])
    mixing_step(3, 0)
    product(pairs[1])
    mixing_step(3, 1)
    arrived(zr, z_sum)
    total = zs[z]
    for d in range(7):
        total = total + zr[d]
    pg[z] = total * (1.0 / (256 * 1024))
    for d in order:
        send("zall", pg.at[z], pg.at[z], at(z=mod(z + d, 8)), z_all)
    mixing_here(3)
    mixing_split(pairs[2])
    mixing_step(4, 0)
    mixing_here(4)
    mixing_split(pairs[3])
    arrived(zr, z_all)

    block = 4 * y_lo + lax.div(z, 2)
    group = 2 * y_lo + core
    po[group] = pg[block]
    outs = next(slots)
    for dy, dc in ((0, 1), (1, 0), (1, 1)):
        to_y, to_core = (flip_y if dy else y), (other_core if dc else core)
        send("out", pg.at[4 * mod(to_y, 2) + lax.div(z, 2)], po.at[group], at(y=to_y, core=to_core), outs)

    p_h, p_l = split(jnp.concatenate([pg[j] for j in range(8)], axis=1))
    for n in range(4):
        cols = pl.ds(256 * n, 256)
        q_own[:, cols] = -dot3(p_h, p_l, m_h[:, cols], m_l[:, cols])
    for n in range(4):
        qa[core, x, y, :, pl.ds(128 * n, 128)] = q_own[:, pl.ds(256 * n, 128)]
        qb[core, y, x, :, pl.ds(128 * n, 128)] = q_own[:, pl.ds(256 * n + 128, 128)]
    q = (qa, qb)
    ones, ups, downs = {}, {}, {}
    across = {(part, off): next(slots) for part in range(2) for off in range(4)}

    def piece(part, off, r):
        return q[part].at[core, mod(first[part] + off, 4), mod(second[part] + r, 4)]

    def q_up(part, off, r):
        ref = piece(part, off, r)
        ups[part, off, r] = send("turn", ref, ref, to_first(part, mod(first[part] + 1, 4)))

    def q_down(part, off, r):
        ref = piece(part, off, r)
        downs[part, off, r] = send("turn", ref, ref, to_first(part, mod(first[part] + 3, 4)))

    def q_pass(part, off, r):
        ref = piece(part, off, r)
        send("across", ref, ref, partner, across[part, off])

    def q_spread(part):
        ref = piece(part, 0, 0)
        for d in (2, 1, 3):
            ones[part, d] = send("ones", ref, ref, to_second(part, mod(second[part] + d, 4)))
        q_up(part, 0, 0)
        q_down(part, 0, 0)
        q_pass(part, 0, 0)

    def q_near(part):
        ones[part, 3].wait_recv()
        q_up(part, 0, 1)
        ones[part, 1].wait_recv()
        q_down(part, 0, 3)
        q_up(part, 0, 3)
        q_pass(part, 0, 1)
        q_pass(part, 0, 3)

    def q_far(part):
        ones[part, 2].wait_recv()
        q_down(part, 0, 2)
        q_up(part, 0, 2)
        q_down(part, 0, 1)
        q_pass(part, 0, 2)

    def q_from_below(part, r):
        ups[part, 0, r].wait_recv()
        if r < 2:
            q_up(part, 3, r)
        q_pass(part, 3, r)

    def q_from_above(part, r):
        downs[part, 0, r].wait_recv()
        if r >= 2:
            q_down(part, 1, r)
        q_pass(part, 1, r)

    def q_opposite(part, *parts):
        for r in parts:
            (ups[part, 3, r] if r < 2 else downs[part, 1, r]).wait_recv()
            q_pass(part, 2, r)

    def q_here(part, off):
        arrived(qa.at[0, 0], across[part, off])

    q_spread(0)
    q_spread(1)
    product(pairs[2])
    product(pairs[3])
    q_near(0)
    q_near(1)
    q_from_below(0, 0)
    q_from_below(1, 0)
    q_from_above(0, 0)
    q_from_above(1, 0)
    q_far(0)
    q_far(1)

    def final(part, off):
        target = mod(first[part] + off, 4)
        if part == 0:
            rows_of_q = jnp.concatenate([qa[c, target, s] for s in range(4) for c in range(2)], axis=0)
            lhs, cols = (psi_h, psi_l), slice(0, 512)
            k0, k1 = aligned(128 * target, 128, 128), aligned(512 + 128 * target, 128, 128)
        else:
            rows_of_q = jnp.concatenate([qb[c, target, s] for s in range(4) for c in range(2)], axis=0)
            lhs, cols = (turn_h, turn_l), slice(512, 1024)
            k0, k1 = aligned(256 * target, 128, 128), aligned(256 * target + 128, 128, 128)
        rhs_h, rhs_l = split(rows_of_q)
        for i in range(4):
            rows = pl.ds(256 * i, 256)
            lhs_h, lhs_l = (jnp.concatenate([ref[rows, k0], ref[rows, k1]], axis=1) for ref in lhs)
            if off == 0:
                start = jnp.concatenate([psi_v[rows, pl.ds(256 * n + 128 * part, 128)] for n in range(4)], axis=1)
            else:
                start = acc[rows, cols]
            acc[rows, cols] = start + dot3(lhs_h, lhs_l, rhs_h, rhs_l)

    q_here(0, 0)
    final(0, 0)
    for part in range(2):
        q_from_below(part, 1)
        q_from_above(part, 3)
    q_here(1, 0)
    final(1, 0)
    for part in range(2):
        q_from_above(part, 2)
        q_from_below(part, 3)
        q_from_below(part, 2)
        q_from_above(part, 1)
    arrived(zr.at[pl.ds(0, 3)], outs)
    proj_v[...] = jnp.transpose(jnp.concatenate([po[j] for j in range(4)], axis=0))
    mine = aligned(32 * (2 * z_odd + core), 32, 32)
    out = pltpu.make_async_copy(proj_v.at[mine], proj_hbm, out_sem.at[0])
    out.start()
    q_here(0, 3)
    final(0, 3)
    q_here(1, 3)
    final(1, 3)
    q_opposite(0, 0, 1)
    q_opposite(1, 0, 1)
    q_here(0, 1)
    final(0, 1)
    q_opposite(0, 3, 2)
    q_opposite(1, 3, 2)
    q_here(1, 1)
    final(1, 1)
    q_here(0, 2)
    final(0, 2)
    q_here(1, 2)
    final(1, 2)
    sizes = (plane_blocks, pr, relay, xr, yr, mg.at[0, pl.ds(0, 7)], mg.at[0], zr, zr, zr.at[pl.ds(0, 3)], yr, pb.at[0, pl.ds(0, 3)], qa)
    for i, ref in enumerate(sizes):
        wait_bytes(ref, send_sem.at[i])
    out.wait()


def body(psi, vpsi, kinetic, mixing):
    anywhere = pl.BlockSpec(memory_space=pl.ANY)
    shapes = [
        ((1024, 1024), F32), ((8, 128), F32), ((8, 128, 128), F32), ((1024, 1024), BF16), ((1024, 1024), BF16),
        ((1024, 1024), BF16), ((1024, 1024), BF16), ((1024, 1024), BF16), ((1024, 1024), BF16), ((1024, 1024), BF16), ((1024, 1024), BF16),
        ((2, 4, 2, 128, 512), F32), ((2, 4, 128, 512), F32), ((2, 2, 64, 512), F32), ((2, 2, 128, 512), F32), ((2, 4, 32, 512), F32),
        ((2, 3, 32, 512), F32), ((8, 32, 128), F32), ((7, 32, 128), F32), ((8, 32, 128), F32), ((4, 32, 128), F32),
        ((2, 8, 2, 8, 32, 128), F32), ((1024, 1024), BF16), ((1024, 1024), BF16),
        ((2, 4, 4, 32, 512), F32), ((2, 4, 4, 32, 512), F32), ((32, 1024), F32), ((128, 128), F32),
    ]
    residual, projected = pl.pallas_call(
        kernel,
        out_shape=(
            pltpu.VMEM((1024, 1024), F32),
            jax.ShapeDtypeStruct((32, 128), F32),
        ),
        in_specs=[anywhere] * 4,
        out_specs=(pl.BlockSpec(memory_space=pltpu.VMEM), anywhere),
        scratch_shapes=[pltpu.VMEM(shape, dtype) for shape, dtype in shapes]
        + [
            pltpu.SemaphoreType.DMA((8,)),
            pltpu.SemaphoreType.DMA((2,)),
            pltpu.SemaphoreType.DMA((len(FAMILIES),)),
            pltpu.SemaphoreType.DMA((SLOTS,)),
        ],
        compiler_params=pltpu.CompilerParams(
            collective_id=0, has_side_effects=True, vmem_limit_bytes=56 * 1024 * 1024
        ),
    )(psi, vpsi, kinetic.reshape(8, 128), mixing.T)
    return residual, projected.T


def solution(mesh):
    placed = (P(("grow", "gcol"), None), P(("grow", "gcol"), None), P(("grow", "gcol")), P("grow", "gcol"))
    return jax.shard_map(
        body,
        mesh=mesh,
        in_specs=placed,
        out_specs=(P(("grow", "gcol"), None), P("grow", "gcol")),
        check_vma=False,
    )
```

```python
import jax
import jax.numpy as jnp
from jax import lax
from jax.experimental import pallas as pl
from jax.experimental.pallas import tpu as pltpu
from jax.sharding import PartitionSpec as P

MESH = pl.DeviceIdType.MESH
F32, BF16 = jnp.float32, jnp.bfloat16
FAMILIES = ("spread", "share", "relay", "direct", "second", "mix", "pass", "zsum", "zall", "out", "ones", "turn", "across")
SLOTS = 83


def split(value):
    high = value.astype(BF16)
    return high, (value - high.astype(F32)).astype(BF16)


def dot(a, b):
    return lax.dot_general(a, b, (((1,), (0,)), ((), ())), preferred_element_type=F32)


def dot3(a_high, a_low, b_high, b_low):
    return dot(a_high, b_high) + dot(a_high, b_low) + dot(a_low, b_high)


def mod(a, n):
    return lax.rem(a, n)


def aligned(start, size, unit):
    return pl.ds(pl.multiple_of(start, unit), size)


def kernel(
    psi_hbm, vpsi_hbm, kin_hbm, mix_hbm, acc, proj_hbm,
    psi_v, kin_v, kin_cols, psi_h, psi_l, turn_h, turn_l, pt_h, pt_l, h_h, h_l,
    pb, pr, relay, xr, own, yr, zs, zr, pg, po, mg, m_h, m_l, qa, qb, q_own, proj_v,
    load_sem, out_sem, send_sem, recv_sem,
):
    row, col = lax.axis_index("grow"), lax.axis_index("gcol")
    x, y_hi = mod(row, 4), lax.div(row, 4)
    core, z, y_lo = mod(col, 2), mod(lax.div(col, 2), 8), lax.div(col, 16)
    y = 2 * y_hi + y_lo
    other_core = 1 - core
    z_odd = mod(z, 2)

    def at(x=x, y=y, z=z, core=core):
        return (4 * lax.div(y, 2) + x, (mod(y, 2) * 8 + z) * 2 + core)

    slots = iter(range(SLOTS))

    def send(family, src, dst, to, slot=None):
        copy = pltpu.make_async_remote_copy(
            src_ref=src,
            dst_ref=dst,
            send_sem=send_sem.at[FAMILIES.index(family)],
            recv_sem=recv_sem.at[next(slots) if slot is None else slot],
            device_id=to,
            device_id_type=MESH,
        )
        copy.start()
        return copy

    def wait_bytes(ref, sem):
        pltpu.make_async_copy(ref, ref, sem).wait()

    def arrived(ref, slot):
        wait_bytes(ref, recv_sem.at[slot])

    own_mix = mg.at[core, z, y_hi, 4 * y_lo + x]
    small = [pltpu.make_async_copy(kin_hbm, kin_v, out_sem.at[0]), pltpu.make_async_copy(mix_hbm, own_mix, out_sem.at[1])]
    for copy in small:
        copy.start()
    for i in range(8):
        rows = pl.ds(128 * i, 128)
        pltpu.make_async_copy(psi_hbm.at[rows], psi_v.at[rows], load_sem.at[i]).start()
        pltpu.make_async_copy(vpsi_hbm.at[rows], acc.at[rows], load_sem.at[i]).start()

    flip_y = y + 1 - 2 * y_lo
    partner = at(core=other_core)
    plane = [at(x=mod(x + dx, 4), y=mod(y + dy, 4)) for dx in range(4) for dy in range(4) if dx + dy > 0]
    peers = [partner, at(y=flip_y, core=other_core)] + plane + [at(z=mod(z + d, 8)) for d in range(1, 8)]
    barrier = pltpu.get_barrier_semaphore()
    for peer in peers:
        pl.semaphore_signal(barrier, inc=1, device_id=peer, device_id_type=MESH)

    for copy in small:
        copy.wait()
    turned = jnp.transpose(jnp.concatenate([kin_v[...]] * 16, axis=0))
    for i in range(8):
        kin_cols[i] = jnp.broadcast_to(turned[:, i : i + 1], (128, 128))

    def prepare(i, carry):
        rows = aligned(128 * i, 128, 128)
        wait_bytes(psi_v.at[pl.ds(0, 256)], load_sem.at[i])
        kin = kin_cols[i]
        for j in range(8):
            cols = pl.ds(128 * j, 128)
            tile = psi_v[rows, cols]
            high, low = split(kin * tile + acc[rows, cols])
            h_h[rows, cols] = high
            h_l[rows, cols] = low
            high, low = split(jnp.transpose(tile))
            pt_h[cols, rows] = high
            pt_l[cols, rows] = low
        return carry

    lax.fori_loop(0, 8, prepare, 0)

    pl.semaphore_wait(barrier, len(peers))

    plane_blocks = pr.at[0, 0, pl.ds(0, 120)]
    spread = next(slots)
    for peer in plane:
        send("spread", own_mix, own_mix, peer, spread)

    passed = [next(slots) for distance in range(5)]

    def mixing_pass(slab, half, distance):
        ref = mg.at[core, slab, half]
        send("pass", ref, ref, partner, passed[distance])

    def mixing_here(distance):
        arrived(mg.at[0, 0] if distance in (0, 4) else mg.at[0, pl.ds(0, 2)], passed[distance])

    def mixing_send(slab, half, step):
        ref = mg.at[core, slab, half]
        return send("mix", ref, ref, at(z=mod(z + step + 8, 8)))

    up, down = {}, {}

    def mixing_start():
        arrived(plane_blocks, spread)
        up[1, 0] = mixing_send(z, 0, 1)
        down[1, 0] = mixing_send(z, 1, -1)
        up[1, 1] = mixing_send(z, 1, 1)
        down[1, 1] = mixing_send(z, 0, -1)
        for half in range(2):
            mixing_pass(z, half, 0)

    def mixing_step(distance, k):
        below, above = mod(z + 8 - distance, 8), mod(z + distance, 8)
        more = distance < 3 or (distance == 3 and k == 0)
        up[distance, k].wait_recv()
        if more:
            up[distance + 1, k] = mixing_send(below, k, 1)
        mixing_pass(below, k, distance)
        down[distance, k].wait_recv()
        if more:
            down[distance + 1, k] = mixing_send(above, 1 - k, -1)
        mixing_pass(above, 1 - k, distance)

    z_pair = lax.div(z, 2)
    pairs = (z_pair, mod(z_pair + 3 + 2 * z_odd, 4), mod(z_pair + 5 - 2 * z_odd, 4), mod(z_pair + 2, 4))

    def mixing_split(pair):
        for half in range(2):
            for k in range(8):
                tile = jnp.concatenate([mg[c, 2 * pair + odd, half, k] for odd in range(2) for c in range(2)], axis=0)
                where = (pl.ds(512 * half + 128 * (k % 4), 128), aligned(256 * pair + 128 * (k // 4), 128, 128))
                high, low = split(jnp.transpose(tile))
                m_h[where] = high
                m_l[where] = low

    def product(pair):
        cols = aligned(256 * pair, 256, 256)

        def rows_of(i, carry):
            rows = aligned(512 * i, 512, 512)
            psi_v[rows, cols] = dot3(h_h[rows, :], h_l[rows, :], m_h[:, cols], m_l[:, cols])
            return carry

        lax.fori_loop(0, 2, rows_of, 0)

    first, second = (x, y), (y, x)

    def to_first(part, f):
        return at(x=f) if part == 0 else at(y=f)

    def to_second(part, s):
        return at(y=s) if part == 0 else at(x=s)

    def share(part, off):
        target = mod(first[part] + off, 4)
        pieces = []
        for half in range(2):
            for s in range(4):
                tx, ty = (target, s) if part == 0 else (s, target)
                start = 512 * lax.div(ty, 2) + 128 * tx + 64 * mod(ty, 2) + 32 * half
                pieces.append(aligned(start, 32, 32))
        lhs_h = jnp.concatenate([pt_h[p, :] for p in pieces], axis=0)
        lhs_l = jnp.concatenate([pt_l[p, :] for p in pieces], axis=0)
        for n in range(2):
            cols = pl.ds(512 * part + 256 * n, 256)
            out = dot3(lhs_h, lhs_l, h_h[:, cols], h_l[:, cols])
            pb[part, off, 0, :, pl.ds(256 * n, 256)] = out[:128]
            pb[part, off, 1, :, pl.ds(256 * n, 256)] = out[128:]
        return send("share", pb.at[part, off, other_core], pr.at[part, off], partner)

    def joined(part, off, copy):
        copy.wait_recv()
        pb[part, off, core] += pr[part, off]

    late, early = pl.ds(0, 64), pl.ds(64, 64)
    relays, direct = {}, {}

    def far(part, copy):
        joined(part, 2, copy)
        f = first[part]
        block = pb.at[part, 2, core]
        relays[part] = (
            send("relay", block.at[late], relay.at[part, 0], to_first(part, mod(f + 1, 4))),
            send("relay", block.at[early], relay.at[part, 1], to_first(part, mod(f + 3, 4))),
        )

    def near(part, off, copy):
        joined(part, off, copy)
        side, rows = (0, early) if off == 1 else (1, late)
        block = pb.at[part, off, core]
        direct[part, off] = next(slots)
        send("direct", block.at[rows], xr.at[part, side, rows], to_first(part, mod(first[part] + off, 4)), direct[part, off])

    def relayed(part, off):
        side, rows = (0, late) if off == 1 else (1, early)
        relays[part][side].wait_recv()
        pb[part, off, core, rows] += relay[part, side]
        block = pb.at[part, off, core]
        send("direct", block.at[rows], xr.at[part, side, rows], to_first(part, mod(first[part] + off, 4)), direct[part, off])

    seconds = {}

    def own_first(part):
        arrived(xr.at[part, 0], direct[part, 1])
        arrived(xr.at[part, 1], direct[part, 3])
        own[part] = (pb[part, 0, core] + xr[part, 0] + xr[part, 1]).reshape(4, 32, 512)
        s = second[part]
        seconds[part] = next(slots)
        for d in (2, 1, 3):
            to = mod(s + d, 4)
            send("second", own.at[part, to], yr.at[part, d - 1], to_second(part, to), seconds[part])

    def own_second(part):
        arrived(yr.at[part], seconds[part])
        total = own[part, second[part]] + yr[part, 0] + yr[part, 1] + yr[part, 2]
        for j in range(4):
            zs[4 * part + j] = total[:, 128 * j : 128 * (j + 1)]

    a2 = share(0, 2)
    b2 = share(1, 2)
    far(0, a2)
    a1 = share(0, 1)
    far(1, b2)
    b1 = share(1, 1)
    near(0, 1, a1)
    a3 = share(0, 3)
    near(1, 1, b1)
    mixing_start()
    b3 = share(1, 3)
    near(0, 3, a3)
    a0 = share(0, 0)
    near(1, 3, b3)
    relayed(0, 1)
    relayed(0, 3)
    b0 = share(1, 0)
    relayed(1, 1)
    relayed(1, 3)
    joined(0, 0, a0)
    joined(1, 0, b0)
    mixing_step(1, 0)

    def natural(i, carry):
        rows = aligned(128 * i, 128, 128)
        high, low = split(psi_v[rows, :])
        psi_h[rows, :] = high
        psi_l[rows, :] = low
        for k in range(4):
            left, right = psi_v[rows, 256 * k : 256 * k + 128], psi_v[rows, 256 * k + 128 : 256 * (k + 1)]
            for yl in range(2):
                lanes = slice(64 * yl, 64 * (yl + 1))
                high, low = split(jnp.concatenate([left[:, lanes], right[:, lanes]], axis=1))
                cols = pl.ds(512 * (k // 2) + 256 * yl + 128 * (k % 2), 128)
                turn_h[rows, cols] = high
                turn_l[rows, cols] = low
        return carry

    lax.fori_loop(0, 5, natural, 0)
    mixing_step(1, 1)
    lax.fori_loop(5, 8, natural, 0)
    own_first(0)
    own_first(1)
    mixing_step(2, 0)
    mixing_here(0)
    mixing_here(1)
    mixing_split(pairs[0])
    product(pairs[0])
    mixing_step(2, 1)
    own_second(0)
    own_second(1)
    order = (4, 3, 5, 2, 6, 1, 7)
    z_sum, z_all = next(slots), next(slots)
    for d in order:
        to = mod(z + d, 8)
        send("zsum", zs.at[to], zr.at[d - 1], at(z=to), z_sum)
    mixing_here(2)
    mixing_split(pairs[1])
    mixing_step(3, 0)
    product(pairs[1])
    arrived(zr, z_sum)
    total = zs[z]
    for d in range(7):
        total = total + zr[d]
    pg[z] = total * (1.0 / (256 * 1024))
    for d in order:
        send("zall", pg.at[z], pg.at[z], at(z=mod(z + d, 8)), z_all)
    mixing_step(3, 1)
    mixing_here(3)
    mixing_split(pairs[2])
    mixing_step(4, 0)
    mixing_here(4)
    mixing_split(pairs[3])
    arrived(zr, z_all)

    block = 4 * y_lo + lax.div(z, 2)
    group = 2 * y_lo + core
    po[group] = pg[block]
    outs = next(slots)
    for dy, dc in ((0, 1), (1, 0), (1, 1)):
        to_y, to_core = (flip_y if dy else y), (other_core if dc else core)
        send("out", pg.at[4 * mod(to_y, 2) + lax.div(z, 2)], po.at[group], at(y=to_y, core=to_core), outs)

    p_h, p_l = split(jnp.concatenate([pg[j] for j in range(8)], axis=1))
    for n in range(4):
        cols = pl.ds(256 * n, 256)
        q_own[:, cols] = -dot3(p_h, p_l, m_h[:, cols], m_l[:, cols])
    for n in range(4):
        qa[core, x, y, :, pl.ds(128 * n, 128)] = q_own[:, pl.ds(256 * n, 128)]
        qb[core, y, x, :, pl.ds(128 * n, 128)] = q_own[:, pl.ds(256 * n + 128, 128)]
    q = (qa, qb)
    ones, ups, downs = {}, {}, {}
    across = {(part, off, k): next(slots) for part in range(2) for off in range(4) for k in range(1 + off % 2)}

    def piece(part, off, r):
        s = mod(second[part] + (r & 2), 4)
        return q[part].at[core, mod(first[part] + off, 4), s + 1 - 2 * mod(s, 2) if r & 1 else s]

    def q_up(part, off, r):
        ref = piece(part, off, r)
        ups[part, off, r] = send("turn", ref, ref, to_first(part, mod(first[part] + 1, 4)))

    def q_down(part, off, r):
        ref = piece(part, off, r)
        downs[part, off, r] = send("turn", ref, ref, to_first(part, mod(first[part] + 3, 4)))

    def q_pass(part, off, r):
        ref = piece(part, off, r)
        send("across", ref, ref, partner, across[part, off, (off & 1) * (r >> 1)])

    def q_spread(part):
        ref = piece(part, 0, 0)
        for d in (2, 1, 3):
            to = mod(second[part] + (d & 2), 4)
            ones[part, d] = send("ones", ref, ref, to_second(part, to + 1 - 2 * mod(to, 2) if d & 1 else to))
        q_up(part, 0, 0)
        q_down(part, 0, 0)
        q_pass(part, 0, 0)

    def q_near(part):
        ones[part, 1].wait_recv()
        q_up(part, 0, 1)
        ones[part, 3].wait_recv()
        q_down(part, 0, 3)
        q_up(part, 0, 3)
        q_down(part, 0, 1)
        q_pass(part, 0, 1)
        q_pass(part, 0, 3)

    def q_far(part):
        ones[part, 2].wait_recv()
        q_down(part, 0, 2)
        q_up(part, 0, 2)
        q_pass(part, 0, 2)

    def q_from_below(part, r):
        ups[part, 0, r].wait_recv()
        if r < 2:
            q_up(part, 3, r)
        q_pass(part, 3, r)

    def q_from_above(part, r):
        downs[part, 0, r].wait_recv()
        if r >= 2:
            q_down(part, 1, r)
        q_pass(part, 1, r)

    def q_opposite(part, *parts):
        for r in parts:
            (ups[part, 3, r] if r < 2 else downs[part, 1, r]).wait_recv()
            q_pass(part, 2, r)

    def q_here(part, off, *k):
        if off % 2 == 0:
            arrived(qa.at[0, 0], across[part, off, 0])
        else:
            arrived(qa.at[0, 0, pl.ds(0, 2)], across[part, off, k[0]])

    q_spread(0)
    q_spread(1)
    product(pairs[2])
    product(pairs[3])
    q_near(0)
    q_near(1)
    q_from_below(0, 0)
    q_from_below(1, 0)
    q_from_above(0, 0)
    q_from_above(1, 0)
    q_far(0)
    q_far(1)

    def final(part, blocks, opening=False):
        lhs, cols = ((psi_h, psi_l), slice(0, 512)) if part == 0 else ((turn_h, turn_l), slice(512, 1024))
        pieces, ks = [], []
        for target, k in blocks:
            pieces += [q[part][c, target, 2 * k + odd] for odd in range(2) for c in range(2)]
            ks.append(aligned(512 * k + 128 * target if part == 0 else 256 * target + 128 * k, 128, 128))
        rhs_h, rhs_l = split(jnp.concatenate(pieces, axis=0))
        for i in range(4):
            rows = pl.ds(256 * i, 256)
            lhs_h, lhs_l = (jnp.concatenate([ref[rows, k] for k in ks], axis=1) for ref in lhs)
            if opening:
                start = jnp.concatenate([psi_v[rows, pl.ds(256 * n + 128 * part, 128)] for n in range(4)], axis=1)
            else:
                start = acc[rows, cols]
            acc[rows, cols] = start + dot3(lhs_h, lhs_l, rhs_h, rhs_l)

    def final_whole(part, off):
        q_here(part, off)
        target = mod(first[part] + off, 4)
        final(part, [(target, 0), (target, 1)], off == 0)

    def final_beside(part, late):
        for off in (3, 1):
            q_here(part, off, late)
        k = mod(lax.div(second[part], 2) + late, 2)
        final(part, [(mod(first[part] + off, 4), k) for off in (3, 1)])

    final_whole(0, 0)
    for part in range(2):
        q_from_below(part, 1)
        q_from_above(part, 3)
    final_whole(1, 0)
    for part in range(2):
        q_from_above(part, 1)
        q_from_above(part, 2)
    final_beside(0, 0)
    for part in range(2):
        q_from_below(part, 3)
        q_from_below(part, 2)
        q_opposite(part, 0, 1, 3)
    final_beside(1, 0)
    arrived(zr.at[pl.ds(0, 3)], outs)
    proj_v[...] = jnp.transpose(jnp.concatenate([po[j] for j in range(4)], axis=0))
    mine = aligned(32 * (2 * z_odd + core), 32, 32)
    out = pltpu.make_async_copy(proj_v.at[mine], proj_hbm, out_sem.at[0])
    out.start()
    final_beside(0, 1)
    q_opposite(0, 2)
    q_opposite(1, 2)
    final_beside(1, 1)
    final_whole(0, 2)
    final_whole(1, 2)
    sizes = (plane_blocks, pr, relay, xr, yr, mg.at[0, pl.ds(0, 7)], mg.at[0], zr, zr, zr.at[pl.ds(0, 3)], yr, pb.at[0, pl.ds(0, 3)], qa)
    for i, ref in enumerate(sizes):
        wait_bytes(ref, send_sem.at[i])
    out.wait()


def body(psi, vpsi, kinetic, mixing):
    anywhere = pl.BlockSpec(memory_space=pl.ANY)
    shapes = [
        ((1024, 1024), F32), ((8, 128), F32), ((8, 128, 128), F32), ((1024, 1024), BF16), ((1024, 1024), BF16),
        ((1024, 1024), BF16), ((1024, 1024), BF16), ((1024, 1024), BF16), ((1024, 1024), BF16), ((1024, 1024), BF16), ((1024, 1024), BF16),
        ((2, 4, 2, 128, 512), F32), ((2, 4, 128, 512), F32), ((2, 2, 64, 512), F32), ((2, 2, 128, 512), F32), ((2, 4, 32, 512), F32),
        ((2, 3, 32, 512), F32), ((8, 32, 128), F32), ((7, 32, 128), F32), ((8, 32, 128), F32), ((4, 32, 128), F32),
        ((2, 8, 2, 8, 32, 128), F32), ((1024, 1024), BF16), ((1024, 1024), BF16),
        ((2, 4, 4, 32, 512), F32), ((2, 4, 4, 32, 512), F32), ((32, 1024), F32), ((128, 128), F32),
    ]
    residual, projected = pl.pallas_call(
        kernel,
        out_shape=(
            pltpu.VMEM((1024, 1024), F32),
            jax.ShapeDtypeStruct((32, 128), F32),
        ),
        in_specs=[anywhere] * 4,
        out_specs=(pl.BlockSpec(memory_space=pltpu.VMEM), anywhere),
        scratch_shapes=[pltpu.VMEM(shape, dtype) for shape, dtype in shapes]
        + [
            pltpu.SemaphoreType.DMA((8,)),
            pltpu.SemaphoreType.DMA((2,)),
            pltpu.SemaphoreType.DMA((len(FAMILIES),)),
            pltpu.SemaphoreType.DMA((SLOTS,)),
        ],
        compiler_params=pltpu.CompilerParams(
            collective_id=0, has_side_effects=True, vmem_limit_bytes=56 * 1024 * 1024
        ),
    )(psi, vpsi, kinetic.reshape(8, 128), mixing.T)
    return residual, projected.T


def solution(mesh):
    placed = (P(("grow", "gcol"), None), P(("grow", "gcol"), None), P(("grow", "gcol")), P("grow", "gcol"))
    return jax.shard_map(
        body,
        mesh=mesh,
        in_specs=placed,
        out_specs=(P(("grow", "gcol"), None), P("grow", "gcol")),
        check_vma=False,
    )
```

```python
import jax
import jax.numpy as jnp
from jax import lax
from jax.experimental import pallas as pl
from jax.experimental.pallas import tpu as pltpu
from jax.sharding import PartitionSpec as P

MESH = pl.DeviceIdType.MESH
F32, BF16 = jnp.float32, jnp.bfloat16
FAMILIES = ("spread", "far", "share", "relay", "direct", "second", "mix", "pass", "zsum", "zall", "out", "ones", "turn", "across")
SLOTS = 83


def split(value):
    high = value.astype(BF16)
    return high, (value - high.astype(F32)).astype(BF16)


def dot(a, b):
    return lax.dot_general(a, b, (((1,), (0,)), ((), ())), preferred_element_type=F32)


def dot3(a_high, a_low, b_high, b_low):
    return dot(a_high, b_high) + dot(a_high, b_low) + dot(a_low, b_high)


def mod(a, n):
    return lax.rem(a, n)


def aligned(start, size, unit):
    return pl.ds(pl.multiple_of(start, unit), size)


def kernel(
    psi_hbm, vpsi_hbm, kin_hbm, mix_hbm, acc, proj_hbm,
    psi_v, kin_v, kin_cols, psi_h, psi_l, turn_h, turn_l, pt_h, pt_l, h_h, h_l,
    pb, pr, relay, xr, own, yr, zs, zr, pg, po, mg, m_h, m_l, qa, qb, q_own, proj_v,
    load_sem, out_sem, send_sem, recv_sem,
):
    row, col = lax.axis_index("grow"), lax.axis_index("gcol")
    x, y_hi = mod(row, 4), lax.div(row, 4)
    core, z, y_lo = mod(col, 2), mod(lax.div(col, 2), 8), lax.div(col, 16)
    y = 2 * y_hi + y_lo
    other_core = 1 - core
    z_odd = mod(z, 2)

    def at(x=x, y=y, z=z, core=core):
        return (4 * lax.div(y, 2) + x, (mod(y, 2) * 8 + z) * 2 + core)

    slots = iter(range(SLOTS))

    def send(family, src, dst, to, slot=None):
        copy = pltpu.make_async_remote_copy(
            src_ref=src,
            dst_ref=dst,
            send_sem=send_sem.at[FAMILIES.index(family)],
            recv_sem=recv_sem.at[next(slots) if slot is None else slot],
            device_id=to,
            device_id_type=MESH,
        )
        copy.start()
        return copy

    def wait_bytes(ref, sem):
        pltpu.make_async_copy(ref, ref, sem).wait()

    def arrived(ref, slot):
        wait_bytes(ref, recv_sem.at[slot])

    own_mix = mg.at[core, z, y_hi, 4 * y_lo + x]
    small = [pltpu.make_async_copy(kin_hbm, kin_v, out_sem.at[0]), pltpu.make_async_copy(mix_hbm, own_mix, out_sem.at[1])]
    for copy in small:
        copy.start()
    for i in range(8):
        rows = pl.ds(128 * i, 128)
        pltpu.make_async_copy(psi_hbm.at[rows], psi_v.at[rows], load_sem.at[i]).start()
        pltpu.make_async_copy(vpsi_hbm.at[rows], acc.at[rows], load_sem.at[i]).start()

    flip_y = y + 1 - 2 * y_lo
    partner = at(core=other_core)
    plane = [at(x=mod(x + dx, 4), y=mod(y + dy, 4)) for dx in range(4) for dy in range(4) if dx + dy > 0]
    peers = [partner, at(y=flip_y, core=other_core)] + plane + [at(z=mod(z + d, 8)) for d in range(1, 8)]
    barrier = pltpu.get_barrier_semaphore()
    for peer in peers:
        pl.semaphore_signal(barrier, inc=1, device_id=peer, device_id_type=MESH)

    for copy in small:
        copy.wait()
    turned = jnp.transpose(jnp.concatenate([kin_v[...]] * 16, axis=0))
    for i in range(8):
        kin_cols[i] = jnp.broadcast_to(turned[:, i : i + 1], (128, 128))

    def prepare(i, carry):
        rows = aligned(128 * i, 128, 128)
        wait_bytes(psi_v.at[pl.ds(0, 256)], load_sem.at[i])
        kin = kin_cols[i]
        for j in range(8):
            cols = pl.ds(128 * j, 128)
            tile = psi_v[rows, cols]
            high, low = split(kin * tile + acc[rows, cols])
            h_h[rows, cols] = high
            h_l[rows, cols] = low
            high, low = split(jnp.transpose(tile))
            pt_h[cols, rows] = high
            pt_l[cols, rows] = low
        return carry

    lax.fori_loop(0, 8, prepare, 0)

    pl.semaphore_wait(barrier, len(peers))

    plane_blocks = pr.at[0, 0, pl.ds(0, 120)]
    spread = next(slots)
    for peer in plane:
        send("spread", own_mix, own_mix, peer, spread)
    across_z = mod(z + 4, 8)
    far_block = send("far", own_mix, own_mix, at(z=across_z))

    passed = [next(slots) for distance in range(5)]
    far_spread = next(slots)

    def mixing_pass(slab, half, distance):
        ref = mg.at[core, slab, half]
        send("pass", ref, ref, partner, passed[distance])

    def mixing_here(distance):
        arrived(mg.at[0, 0] if distance in (0, 4) else mg.at[0, pl.ds(0, 2)], passed[distance])

    def mixing_send(slab, half, step):
        ref = mg.at[core, slab, half]
        return send("mix", ref, ref, at(z=mod(z + step + 8, 8)))

    up, down = {}, {}

    def mixing_start():
        arrived(plane_blocks, spread)
        up[1, 0] = mixing_send(z, 0, 1)
        down[1, 0] = mixing_send(z, 1, -1)
        up[1, 1] = mixing_send(z, 1, 1)
        down[1, 1] = mixing_send(z, 0, -1)
        for half in range(2):
            mixing_pass(z, half, 0)

    def mixing_forward(distance, k):
        below, above = mod(z + 8 - distance, 8), mod(z + distance, 8)
        up[distance + 1, k] = mixing_send(below, k, 1)
        down[distance + 1, k] = mixing_send(above, 1 - k, -1)

    def mixing_step(distance, k, forward=True):
        below, above = mod(z + 8 - distance, 8), mod(z + distance, 8)
        up[distance, k].wait_recv()
        if forward:
            up[distance + 1, k] = mixing_send(below, k, 1)
        mixing_pass(below, k, distance)
        down[distance, k].wait_recv()
        if forward:
            down[distance + 1, k] = mixing_send(above, 1 - k, -1)
        mixing_pass(above, 1 - k, distance)

    def mixing_far_start():
        far_block.wait_recv()
        ref = mg.at[core, across_z, y_hi, 4 * y_lo + x]
        for peer in plane:
            send("spread", ref, ref, peer, far_spread)

    def mixing_far_pass():
        arrived(plane_blocks, far_spread)
        for half in range(2):
            mixing_pass(across_z, half, 4)

    z_pair = lax.div(z, 2)
    pairs = (z_pair, mod(z_pair + 3 + 2 * z_odd, 4), mod(z_pair + 5 - 2 * z_odd, 4), mod(z_pair + 2, 4))

    def mixing_split(pair):
        for half in range(2):
            for k in range(8):
                tile = jnp.concatenate([mg[c, 2 * pair + odd, half, k] for odd in range(2) for c in range(2)], axis=0)
                where = (pl.ds(512 * half + 128 * (k % 4), 128), aligned(256 * pair + 128 * (k // 4), 128, 128))
                high, low = split(jnp.transpose(tile))
                m_h[where] = high
                m_l[where] = low

    def product(pair):
        cols = aligned(256 * pair, 256, 256)

        def rows_of(i, carry):
            rows = aligned(512 * i, 512, 512)
            psi_v[rows, cols] = dot3(h_h[rows, :], h_l[rows, :], m_h[:, cols], m_l[:, cols])
            return carry

        lax.fori_loop(0, 2, rows_of, 0)

    first, second = (x, y), (y, x)

    def to_first(part, f):
        return at(x=f) if part == 0 else at(y=f)

    def to_second(part, s):
        return at(y=s) if part == 0 else at(x=s)

    def share(part, off):
        target = mod(first[part] + off, 4)
        pieces = []
        for half in range(2):
            for s in range(4):
                tx, ty = (target, s) if part == 0 else (s, target)
                start = 512 * lax.div(ty, 2) + 128 * tx + 64 * mod(ty, 2) + 32 * half
                pieces.append(aligned(start, 32, 32))
        lhs_h = jnp.concatenate([pt_h[p, :] for p in pieces], axis=0)
        lhs_l = jnp.concatenate([pt_l[p, :] for p in pieces], axis=0)
        for n in range(2):
            cols = pl.ds(512 * part + 256 * n, 256)
            out = dot3(lhs_h, lhs_l, h_h[:, cols], h_l[:, cols])
            pb[part, off, 0, :, pl.ds(256 * n, 256)] = out[:128]
            pb[part, off, 1, :, pl.ds(256 * n, 256)] = out[128:]
        return send("share", pb.at[part, off, other_core], pr.at[part, off], partner)

    def joined(part, off, copy):
        copy.wait_recv()
        pb[part, off, core] += pr[part, off]

    late, early = pl.ds(0, 64), pl.ds(64, 64)
    relays, direct = {}, {}

    def far(part, copy):
        joined(part, 2, copy)
        f = first[part]
        block = pb.at[part, 2, core]
        relays[part] = (
            send("relay", block.at[late], relay.at[part, 0], to_first(part, mod(f + 1, 4))),
            send("relay", block.at[early], relay.at[part, 1], to_first(part, mod(f + 3, 4))),
        )

    def near(part, off, copy):
        joined(part, off, copy)
        side, rows = (0, early) if off == 1 else (1, late)
        block = pb.at[part, off, core]
        direct[part, off] = next(slots)
        send("direct", block.at[rows], xr.at[part, side, rows], to_first(part, mod(first[part] + off, 4)), direct[part, off])

    def relayed(part, off):
        side, rows = (0, late) if off == 1 else (1, early)
        relays[part][side].wait_recv()
        pb[part, off, core, rows] += relay[part, side]
        block = pb.at[part, off, core]
        send("direct", block.at[rows], xr.at[part, side, rows], to_first(part, mod(first[part] + off, 4)), direct[part, off])

    seconds = {}

    def own_first(part):
        arrived(xr.at[part, 0], direct[part, 1])
        arrived(xr.at[part, 1], direct[part, 3])
        own[part] = (pb[part, 0, core] + xr[part, 0] + xr[part, 1]).reshape(4, 32, 512)
        s = second[part]
        seconds[part] = next(slots)
        for d in (2, 1, 3):
            to = mod(s + d, 4)
            send("second", own.at[part, to], yr.at[part, d - 1], to_second(part, to), seconds[part])

    def own_second(part):
        arrived(yr.at[part], seconds[part])
        total = own[part, second[part]] + yr[part, 0] + yr[part, 1] + yr[part, 2]
        for j in range(4):
            zs[4 * part + j] = total[:, 128 * j : 128 * (j + 1)]

    a2 = share(0, 2)
    b2 = share(1, 2)
    far(0, a2)
    a1 = share(0, 1)
    far(1, b2)
    b1 = share(1, 1)
    near(0, 1, a1)
    a3 = share(0, 3)
    near(1, 1, b1)
    mixing_start()
    b3 = share(1, 3)
    near(0, 3, a3)
    a0 = share(0, 0)
    near(1, 3, b3)
    relayed(0, 1)
    relayed(0, 3)
    b0 = share(1, 0)
    relayed(1, 1)
    relayed(1, 3)
    joined(0, 0, a0)
    joined(1, 0, b0)
    mixing_step(1, 0)

    def natural(i, carry):
        rows = aligned(128 * i, 128, 128)
        high, low = split(psi_v[rows, :])
        psi_h[rows, :] = high
        psi_l[rows, :] = low
        for k in range(4):
            left, right = psi_v[rows, 256 * k : 256 * k + 128], psi_v[rows, 256 * k + 128 : 256 * (k + 1)]
            for yl in range(2):
                lanes = slice(64 * yl, 64 * (yl + 1))
                high, low = split(jnp.concatenate([left[:, lanes], right[:, lanes]], axis=1))
                cols = pl.ds(512 * (k // 2) + 256 * yl + 128 * (k % 2), 128)
                turn_h[rows, cols] = high
                turn_l[rows, cols] = low
        return carry

    lax.fori_loop(0, 5, natural, 0)
    mixing_step(1, 1)
    lax.fori_loop(5, 8, natural, 0)
    own_first(0)
    own_first(1)
    mixing_step(2, 0)
    mixing_here(0)
    mixing_here(1)
    mixing_split(pairs[0])
    product(pairs[0])
    mixing_step(2, 1, forward=False)
    own_second(0)
    own_second(1)
    order = (4, 3, 5, 2, 6, 1, 7)
    z_sum, z_all = next(slots), next(slots)
    for d in order:
        to = mod(z + d, 8)
        send("zsum", zs.at[to], zr.at[d - 1], at(z=to), z_sum)
    mixing_forward(2, 1)
    mixing_far_start()
    mixing_here(2)
    mixing_split(pairs[1])
    mixing_step(3, 0, forward=False)
    product(pairs[1])
    arrived(zr, z_sum)
    total = zs[z]
    for d in range(7):
        total = total + zr[d]
    pg[z] = total * (1.0 / (256 * 1024))
    for d in order:
        send("zall", pg.at[z], pg.at[z], at(z=mod(z + d, 8)), z_all)
    mixing_far_pass()
    mixing_step(3, 1, forward=False)
    mixing_here(3)
    mixing_split(pairs[2])
    mixing_here(4)
    mixing_split(pairs[3])
    arrived(zr, z_all)

    block = 4 * y_lo + lax.div(z, 2)
    group = 2 * y_lo + core
    po[group] = pg[block]
    outs = next(slots)
    for dy, dc in ((0, 1), (1, 0), (1, 1)):
        to_y, to_core = (flip_y if dy else y), (other_core if dc else core)
        send("out", pg.at[4 * mod(to_y, 2) + lax.div(z, 2)], po.at[group], at(y=to_y, core=to_core), outs)

    p_h, p_l = split(jnp.concatenate([pg[j] for j in range(8)], axis=1))
    for n in range(4):
        cols = pl.ds(256 * n, 256)
        q_own[:, cols] = -dot3(p_h, p_l, m_h[:, cols], m_l[:, cols])
    for n in range(4):
        qa[core, x, y, :, pl.ds(128 * n, 128)] = q_own[:, pl.ds(256 * n, 128)]
        qb[core, y, x, :, pl.ds(128 * n, 128)] = q_own[:, pl.ds(256 * n + 128, 128)]
    q = (qa, qb)
    ones, ups, downs = {}, {}, {}
    across = {(part, off, k): next(slots) for part in range(2) for off in range(4) for k in range(1 + off % 2)}

    def piece(part, off, r):
        s = mod(second[part] + (r & 2), 4)
        return q[part].at[core, mod(first[part] + off, 4), s + 1 - 2 * mod(s, 2) if r & 1 else s]

    def q_up(part, off, r):
        ref = piece(part, off, r)
        ups[part, off, r] = send("turn", ref, ref, to_first(part, mod(first[part] + 1, 4)))

    def q_down(part, off, r):
        ref = piece(part, off, r)
        downs[part, off, r] = send("turn", ref, ref, to_first(part, mod(first[part] + 3, 4)))

    def q_pass(part, off, r):
        ref = piece(part, off, r)
        send("across", ref, ref, partner, across[part, off, (off & 1) * (r >> 1)])

    def q_spread(part):
        ref = piece(part, 0, 0)
        for d in (2, 1, 3):
            to = mod(second[part] + (d & 2), 4)
            ones[part, d] = send("ones", ref, ref, to_second(part, to + 1 - 2 * mod(to, 2) if d & 1 else to))

    def q_first(part):
        q_up(part, 0, 0)
        q_down(part, 0, 0)
        q_pass(part, 0, 0)

    def q_near(part):
        ones[part, 1].wait_recv()
        q_up(part, 0, 1)
        q_down(part, 0, 1)
        ones[part, 3].wait_recv()
        q_down(part, 0, 3)
        q_up(part, 0, 3)
        q_pass(part, 0, 1)
        q_pass(part, 0, 3)

    def q_far(part):
        ones[part, 2].wait_recv()
        q_down(part, 0, 2)
        q_up(part, 0, 2)
        q_pass(part, 0, 2)

    def q_from_below(part, r):
        ups[part, 0, r].wait_recv()
        if r < 2:
            q_up(part, 3, r)
        q_pass(part, 3, r)

    def q_from_above(part, r):
        downs[part, 0, r].wait_recv()
        if r >= 2:
            q_down(part, 1, r)
        q_pass(part, 1, r)

    def q_opposite(part, *parts):
        for r in parts:
            (ups[part, 3, r] if r < 2 else downs[part, 1, r]).wait_recv()
            q_pass(part, 2, r)

    def q_here(part, off, *k):
        if off % 2 == 0:
            arrived(qa.at[0, 0], across[part, off, 0])
        else:
            arrived(qa.at[0, 0, pl.ds(0, 2)], across[part, off, k[0]])

    q_spread(0)
    q_spread(1)
    q_first(0)
    q_first(1)
    product(pairs[2])
    product(pairs[3])
    q_near(0)
    q_near(1)
    q_from_below(0, 0)
    q_from_below(1, 0)
    q_from_above(0, 0)
    q_from_above(1, 0)
    q_far(0)
    q_far(1)

    def final(part, blocks, opening=False):
        lhs, cols = ((psi_h, psi_l), slice(0, 512)) if part == 0 else ((turn_h, turn_l), slice(512, 1024))
        pieces, ks = [], []
        for target, k in blocks:
            pieces += [q[part][c, target, 2 * k + odd] for odd in range(2) for c in range(2)]
            ks.append(aligned(512 * k + 128 * target if part == 0 else 256 * target + 128 * k, 128, 128))
        rhs_h, rhs_l = split(jnp.concatenate(pieces, axis=0))
        for i in range(4):
            rows = pl.ds(256 * i, 256)
            lhs_h, lhs_l = (jnp.concatenate([ref[rows, k] for k in ks], axis=1) for ref in lhs)
            if opening:
                start = jnp.concatenate([psi_v[rows, pl.ds(256 * n + 128 * part, 128)] for n in range(4)], axis=1)
            else:
                start = acc[rows, cols]
            acc[rows, cols] = start + dot3(lhs_h, lhs_l, rhs_h, rhs_l)

    def final_whole(part, off):
        q_here(part, off)
        target = mod(first[part] + off, 4)
        final(part, [(target, 0), (target, 1)], off == 0)

    def final_beside(part, late):
        for off in (3, 1):
            q_here(part, off, late)
        k = mod(lax.div(second[part], 2) + late, 2)
        final(part, [(mod(first[part] + off, 4), k) for off in (3, 1)])

    final_whole(0, 0)
    for part in range(2):
        q_from_below(part, 1)
        q_from_above(part, 1)
    for part in range(2):
        q_from_above(part, 3)
    final_whole(1, 0)
    final_beside(0, 0)
    for part in range(2):
        q_from_above(part, 2)
    final_beside(1, 0)
    for part in range(2):
        q_from_below(part, 3)
        q_from_below(part, 2)
    for part in range(2):
        q_opposite(part, 0, 1, 3)
    arrived(zr.at[pl.ds(0, 3)], outs)
    proj_v[...] = jnp.transpose(jnp.concatenate([po[j] for j in range(4)], axis=0))
    mine = aligned(32 * (2 * z_odd + core), 32, 32)
    out = pltpu.make_async_copy(proj_v.at[mine], proj_hbm, out_sem.at[0])
    out.start()
    final_beside(0, 1)
    q_opposite(0, 2)
    q_opposite(1, 2)
    final_beside(1, 1)
    final_whole(0, 2)
    final_whole(1, 2)
    sizes = (pr.at[0, pl.ds(0, 2), pl.ds(0, 120)], zr.at[0], pr, relay, xr, yr, mg.at[0, pl.ds(0, 6)], mg.at[0], zr, zr, zr.at[pl.ds(0, 3)], yr, pb.at[0, pl.ds(0, 3)], qa)
    for i, ref in enumerate(sizes):
        wait_bytes(ref, send_sem.at[i])
    out.wait()


def body(psi, vpsi, kinetic, mixing):
    anywhere = pl.BlockSpec(memory_space=pl.ANY)
    shapes = [
        ((1024, 1024), F32), ((8, 128), F32), ((8, 128, 128), F32), ((1024, 1024), BF16), ((1024, 1024), BF16),
        ((1024, 1024), BF16), ((1024, 1024), BF16), ((1024, 1024), BF16), ((1024, 1024), BF16), ((1024, 1024), BF16), ((1024, 1024), BF16),
        ((2, 4, 2, 128, 512), F32), ((2, 4, 128, 512), F32), ((2, 2, 64, 512), F32), ((2, 2, 128, 512), F32), ((2, 4, 32, 512), F32),
        ((2, 3, 32, 512), F32), ((8, 32, 128), F32), ((7, 32, 128), F32), ((8, 32, 128), F32), ((4, 32, 128), F32),
        ((2, 8, 2, 8, 32, 128), F32), ((1024, 1024), BF16), ((1024, 1024), BF16),
        ((2, 4, 4, 32, 512), F32), ((2, 4, 4, 32, 512), F32), ((32, 1024), F32), ((128, 128), F32),
    ]
    residual, projected = pl.pallas_call(
        kernel,
        out_shape=(
            pltpu.VMEM((1024, 1024), F32),
            jax.ShapeDtypeStruct((32, 128), F32),
        ),
        in_specs=[anywhere] * 4,
        out_specs=(pl.BlockSpec(memory_space=pltpu.VMEM), anywhere),
        scratch_shapes=[pltpu.VMEM(shape, dtype) for shape, dtype in shapes]
        + [
            pltpu.SemaphoreType.DMA((8,)),
            pltpu.SemaphoreType.DMA((2,)),
            pltpu.SemaphoreType.DMA((len(FAMILIES),)),
            pltpu.SemaphoreType.DMA((SLOTS,)),
        ],
        compiler_params=pltpu.CompilerParams(
            collective_id=0, has_side_effects=True, vmem_limit_bytes=56 * 1024 * 1024
        ),
    )(psi, vpsi, kinetic.reshape(8, 128), mixing.T)
    return residual, projected.T


def solution(mesh):
    placed = (P(("grow", "gcol"), None), P(("grow", "gcol"), None), P(("grow", "gcol")), P("grow", "gcol"))
    return jax.shard_map(
        body,
        mesh=mesh,
        in_specs=placed,
        out_specs=(P(("grow", "gcol"), None), P("grow", "gcol")),
        check_vma=False,
    )
```

```python
import jax
import jax.numpy as jnp
from jax import lax
from jax.experimental import pallas as pl
from jax.experimental.pallas import tpu as pltpu
from jax.sharding import PartitionSpec as P

MESH = pl.DeviceIdType.MESH
F32, BF16 = jnp.float32, jnp.bfloat16
FAMILIES = ("spread", "far", "share", "relay", "direct", "second", "mix", "pass", "zsum", "zall", "out", "ones", "turn", "across")
SLOTS = 83


def split(value):
    high = value.astype(BF16)
    return high, (value - high.astype(F32)).astype(BF16)


def dot(a, b):
    return lax.dot_general(a, b, (((1,), (0,)), ((), ())), preferred_element_type=F32)


def dot3(a_high, a_low, b_high, b_low):
    return dot(a_high, b_high) + dot(a_high, b_low) + dot(a_low, b_high)


def mod(a, n):
    return lax.rem(a, n)


def aligned(start, size, unit):
    return pl.ds(pl.multiple_of(start, unit), size)


def kernel(
    psi_hbm, vpsi_hbm, kin_hbm, mix_hbm, acc, proj_hbm,
    psi_v, kin_v, kin_cols, psi_h, psi_l, turn_h, turn_l, pt_h, pt_l, h_h, h_l,
    pb, pr, relay, xr, own, yr, zs, zr, pg, po, mg, m_h, m_l, qa, qb, q_own, proj_v,
    load_sem, out_sem, send_sem, recv_sem,
):
    row, col = lax.axis_index("grow"), lax.axis_index("gcol")
    x, y_hi = mod(row, 4), lax.div(row, 4)
    core, z, y_lo = mod(col, 2), mod(lax.div(col, 2), 8), lax.div(col, 16)
    y = 2 * y_hi + y_lo
    other_core = 1 - core
    z_odd = mod(z, 2)

    def at(x=x, y=y, z=z, core=core):
        return (4 * lax.div(y, 2) + x, (mod(y, 2) * 8 + z) * 2 + core)

    slots = iter(range(SLOTS))

    def send(family, src, dst, to, slot=None):
        copy = pltpu.make_async_remote_copy(
            src_ref=src,
            dst_ref=dst,
            send_sem=send_sem.at[FAMILIES.index(family)],
            recv_sem=recv_sem.at[next(slots) if slot is None else slot],
            device_id=to,
            device_id_type=MESH,
        )
        copy.start()
        return copy

    def wait_bytes(ref, sem):
        pltpu.make_async_copy(ref, ref, sem).wait()

    def arrived(ref, slot):
        wait_bytes(ref, recv_sem.at[slot])

    own_mix = mg.at[core, z, y_hi, 4 * y_lo + x]
    small = [pltpu.make_async_copy(kin_hbm, kin_v, out_sem.at[0]), pltpu.make_async_copy(mix_hbm, own_mix, out_sem.at[1])]
    for copy in small:
        copy.start()
    for i in range(8):
        rows = pl.ds(128 * i, 128)
        pltpu.make_async_copy(psi_hbm.at[rows], psi_v.at[rows], load_sem.at[i]).start()
        pltpu.make_async_copy(vpsi_hbm.at[rows], acc.at[rows], load_sem.at[i]).start()

    flip_y = y + 1 - 2 * y_lo
    partner = at(core=other_core)
    plane = [at(x=mod(x + dx, 4), y=mod(y + dy, 4)) for dx in range(4) for dy in range(4) if dx + dy > 0]
    peers = [partner, at(y=flip_y, core=other_core)] + plane + [at(z=mod(z + d, 8)) for d in range(1, 8)]
    barrier = pltpu.get_barrier_semaphore()
    for peer in peers:
        pl.semaphore_signal(barrier, inc=1, device_id=peer, device_id_type=MESH)

    for copy in small:
        copy.wait()
    turned = jnp.transpose(jnp.concatenate([kin_v[...]] * 16, axis=0))
    for i in range(8):
        kin_cols[i] = jnp.broadcast_to(turned[:, i : i + 1], (128, 128))

    def prepare(i, carry):
        rows = aligned(128 * i, 128, 128)
        wait_bytes(psi_v.at[pl.ds(0, 256)], load_sem.at[i])
        kin = kin_cols[i]
        for j in range(8):
            cols = pl.ds(128 * j, 128)
            tile = psi_v[rows, cols]
            high, low = split(kin * tile + acc[rows, cols])
            h_h[rows, cols] = high
            h_l[rows, cols] = low
            high, low = split(jnp.transpose(tile))
            pt_h[cols, rows] = high
            pt_l[cols, rows] = low
        return carry

    lax.fori_loop(0, 8, prepare, 0)

    pl.semaphore_wait(barrier, len(peers))

    plane_blocks = pr.at[0, 0, pl.ds(0, 120)]
    spread = next(slots)
    for peer in plane:
        send("spread", own_mix, own_mix, peer, spread)
    across_z = mod(z + 4, 8)
    far_block = send("far", own_mix, own_mix, at(z=across_z))

    passed = [next(slots) for distance in range(5)]
    far_spread = next(slots)

    def mixing_pass(slab, half, distance):
        ref = mg.at[core, slab, half]
        send("pass", ref, ref, partner, passed[distance])

    def mixing_here(distance):
        arrived(mg.at[0, 0] if distance in (0, 4) else mg.at[0, pl.ds(0, 2)], passed[distance])

    def mixing_send(slab, half, step):
        ref = mg.at[core, slab, half]
        return send("mix", ref, ref, at(z=mod(z + step + 8, 8)))

    up, down = {}, {}

    def mixing_start():
        arrived(plane_blocks, spread)
        up[1, 0] = mixing_send(z, 0, 1)
        down[1, 0] = mixing_send(z, 1, -1)
        up[1, 1] = mixing_send(z, 1, 1)
        down[1, 1] = mixing_send(z, 0, -1)
        for half in range(2):
            mixing_pass(z, half, 0)

    def mixing_forward(distance, k):
        below, above = mod(z + 8 - distance, 8), mod(z + distance, 8)
        up[distance + 1, k] = mixing_send(below, k, 1)
        down[distance + 1, k] = mixing_send(above, 1 - k, -1)

    def mixing_step(distance, k, forward=True):
        below, above = mod(z + 8 - distance, 8), mod(z + distance, 8)
        up[distance, k].wait_recv()
        if forward:
            up[distance + 1, k] = mixing_send(below, k, 1)
        mixing_pass(below, k, distance)
        down[distance, k].wait_recv()
        if forward:
            down[distance + 1, k] = mixing_send(above, 1 - k, -1)
        mixing_pass(above, 1 - k, distance)

    def mixing_far_start():
        far_block.wait_recv()
        ref = mg.at[core, across_z, y_hi, 4 * y_lo + x]
        for peer in plane:
            send("spread", ref, ref, peer, far_spread)

    def mixing_far_pass():
        arrived(plane_blocks, far_spread)
        for half in range(2):
            mixing_pass(across_z, half, 4)

    z_pair = lax.div(z, 2)
    pairs = (z_pair, mod(z_pair + 3 + 2 * z_odd, 4), mod(z_pair + 5 - 2 * z_odd, 4), mod(z_pair + 2, 4))

    def mixing_split(pair):
        for half in range(2):
            for k in range(8):
                tile = jnp.concatenate([mg[c, 2 * pair + odd, half, k] for odd in range(2) for c in range(2)], axis=0)
                where = (pl.ds(512 * half + 128 * (k % 4), 128), aligned(256 * pair + 128 * (k // 4), 128, 128))
                high, low = split(jnp.transpose(tile))
                m_h[where] = high
                m_l[where] = low

    def product(pair):
        cols = aligned(256 * pair, 256, 256)

        def rows_of(i, carry):
            rows = aligned(512 * i, 512, 512)
            psi_v[rows, cols] = dot3(h_h[rows, :], h_l[rows, :], m_h[:, cols], m_l[:, cols])
            return carry

        lax.fori_loop(0, 2, rows_of, 0)

    first, second = (x, y), (y, x)

    def to_first(part, f):
        return at(x=f) if part == 0 else at(y=f)

    def to_second(part, s):
        return at(y=s) if part == 0 else at(x=s)

    def share(part, off):
        target = mod(first[part] + off, 4)
        pieces = []
        for half in range(2):
            for s in range(4):
                tx, ty = (target, s) if part == 0 else (s, target)
                start = 512 * lax.div(ty, 2) + 128 * tx + 64 * mod(ty, 2) + 32 * half
                pieces.append(aligned(start, 32, 32))
        lhs_h = jnp.concatenate([pt_h[p, :] for p in pieces], axis=0)
        lhs_l = jnp.concatenate([pt_l[p, :] for p in pieces], axis=0)
        for n in range(2):
            cols = pl.ds(512 * part + 256 * n, 256)
            out = dot3(lhs_h, lhs_l, h_h[:, cols], h_l[:, cols])
            pb[part, off, 0, :, pl.ds(256 * n, 256)] = out[:128]
            pb[part, off, 1, :, pl.ds(256 * n, 256)] = out[128:]
        return send("share", pb.at[part, off, other_core], pr.at[part, off], partner)

    def joined(part, off, copy):
        copy.wait_recv()
        pb[part, off, core] += pr[part, off]

    late, early = pl.ds(0, 64), pl.ds(64, 64)
    relays, direct = {}, {}

    def far(part, copy):
        joined(part, 2, copy)
        f = first[part]
        block = pb.at[part, 2, core]
        relays[part] = (
            send("relay", block.at[late], relay.at[part, 0], to_first(part, mod(f + 1, 4))),
            send("relay", block.at[early], relay.at[part, 1], to_first(part, mod(f + 3, 4))),
        )

    def near(part, off, copy):
        joined(part, off, copy)
        side, rows = (0, early) if off == 1 else (1, late)
        block = pb.at[part, off, core]
        direct[part, off] = next(slots)
        send("direct", block.at[rows], xr.at[part, side, rows], to_first(part, mod(first[part] + off, 4)), direct[part, off])

    def relayed(part, off):
        side, rows = (0, late) if off == 1 else (1, early)
        relays[part][side].wait_recv()
        pb[part, off, core, rows] += relay[part, side]
        block = pb.at[part, off, core]
        send("direct", block.at[rows], xr.at[part, side, rows], to_first(part, mod(first[part] + off, 4)), direct[part, off])

    seconds = {}

    def own_first(part):
        arrived(xr.at[part, 0], direct[part, 1])
        arrived(xr.at[part, 1], direct[part, 3])
        own[part] = (pb[part, 0, core] + xr[part, 0] + xr[part, 1]).reshape(4, 32, 512)
        s = second[part]
        seconds[part] = next(slots)
        for d in (2, 1, 3):
            to = mod(s + d, 4)
            send("second", own.at[part, to], yr.at[part, d - 1], to_second(part, to), seconds[part])

    def own_second(part):
        arrived(yr.at[part], seconds[part])
        total = own[part, second[part]] + yr[part, 0] + yr[part, 1] + yr[part, 2]
        for j in range(4):
            zs[4 * part + j] = total[:, 128 * j : 128 * (j + 1)]

    a2 = share(0, 2)
    b2 = share(1, 2)
    far(0, a2)
    a1 = share(0, 1)
    far(1, b2)
    a3 = share(0, 3)
    near(0, 1, a1)
    b1 = share(1, 1)
    near(0, 3, a3)
    mixing_start()
    b3 = share(1, 3)
    near(1, 1, b1)
    relayed(0, 1)
    relayed(0, 3)
    a0 = share(0, 0)
    near(1, 3, b3)
    relayed(1, 1)
    relayed(1, 3)
    b0 = share(1, 0)
    joined(0, 0, a0)
    joined(1, 0, b0)
    mixing_step(1, 0)

    def natural(i, carry):
        rows = aligned(128 * i, 128, 128)
        high, low = split(psi_v[rows, :])
        psi_h[rows, :] = high
        psi_l[rows, :] = low
        for k in range(4):
            left, right = psi_v[rows, 256 * k : 256 * k + 128], psi_v[rows, 256 * k + 128 : 256 * (k + 1)]
            for yl in range(2):
                lanes = slice(64 * yl, 64 * (yl + 1))
                high, low = split(jnp.concatenate([left[:, lanes], right[:, lanes]], axis=1))
                cols = pl.ds(512 * (k // 2) + 256 * yl + 128 * (k % 2), 128)
                turn_h[rows, cols] = high
                turn_l[rows, cols] = low
        return carry

    lax.fori_loop(0, 5, natural, 0)
    mixing_step(1, 1)
    lax.fori_loop(5, 8, natural, 0)
    own_first(0)
    own_first(1)
    mixing_step(2, 0)
    mixing_here(0)
    mixing_here(1)
    mixing_split(pairs[0])
    product(pairs[0])
    mixing_step(2, 1, forward=False)
    own_second(0)
    own_second(1)
    order = (4, 3, 5, 2, 6, 1, 7)
    z_sum, z_all = next(slots), next(slots)
    for d in order:
        to = mod(z + d, 8)
        send("zsum", zs.at[to], zr.at[d - 1], at(z=to), z_sum)
    mixing_forward(2, 1)
    mixing_far_start()
    mixing_here(2)
    mixing_split(pairs[1])
    mixing_step(3, 0, forward=False)
    product(pairs[1])
    arrived(zr, z_sum)
    total = zs[z]
    for d in range(7):
        total = total + zr[d]
    pg[z] = total * (1.0 / (256 * 1024))
    for d in order:
        send("zall", pg.at[z], pg.at[z], at(z=mod(z + d, 8)), z_all)
    mixing_far_pass()
    mixing_step(3, 1, forward=False)
    mixing_here(3)
    mixing_split(pairs[2])
    mixing_here(4)
    mixing_split(pairs[3])
    arrived(zr, z_all)

    block = 4 * y_lo + lax.div(z, 2)
    group = 2 * y_lo + core
    po[group] = pg[block]
    outs = next(slots)
    for dy, dc in ((0, 1), (1, 0), (1, 1)):
        to_y, to_core = (flip_y if dy else y), (other_core if dc else core)
        send("out", pg.at[4 * mod(to_y, 2) + lax.div(z, 2)], po.at[group], at(y=to_y, core=to_core), outs)

    p_h, p_l = split(jnp.concatenate([pg[j] for j in range(8)], axis=1))
    p_both = jnp.concatenate([p_h, p_l], axis=0)
    for n in range(4):
        cols = pl.ds(256 * n, 256)
        both = dot(p_both, m_h[:, cols])
        q_own[:, cols] = -(both[:32] + dot(p_h, m_l[:, cols]) + both[32:])
    for n in range(4):
        qa[core, x, y, :, pl.ds(128 * n, 128)] = q_own[:, pl.ds(256 * n, 128)]
        qb[core, y, x, :, pl.ds(128 * n, 128)] = q_own[:, pl.ds(256 * n + 128, 128)]
    q = (qa, qb)
    ones, ups, downs = {}, {}, {}
    across = {(part, off, k): next(slots) for part in range(2) for off in range(4) for k in range(1 + off % 2)}

    def piece(part, off, r):
        s = mod(second[part] + (r & 2), 4)
        return q[part].at[core, mod(first[part] + off, 4), s + 1 - 2 * mod(s, 2) if r & 1 else s]

    def q_up(part, off, r):
        ref = piece(part, off, r)
        ups[part, off, r] = send("turn", ref, ref, to_first(part, mod(first[part] + 1, 4)))

    def q_down(part, off, r):
        ref = piece(part, off, r)
        downs[part, off, r] = send("turn", ref, ref, to_first(part, mod(first[part] + 3, 4)))

    def q_pass(part, off, r):
        ref = piece(part, off, r)
        send("across", ref, ref, partner, across[part, off, (off & 1) * (r >> 1)])

    def q_spread(part):
        ref = piece(part, 0, 0)
        for d in (2, 1, 3):
            to = mod(second[part] + (d & 2), 4)
            ones[part, d] = send("ones", ref, ref, to_second(part, to + 1 - 2 * mod(to, 2) if d & 1 else to))

    def q_first(part):
        q_up(part, 0, 0)
        q_down(part, 0, 0)
        q_pass(part, 0, 0)

    def q_near(part):
        ones[part, 1].wait_recv()
        q_up(part, 0, 1)
        q_down(part, 0, 1)
        ones[part, 3].wait_recv()
        q_down(part, 0, 3)
        q_up(part, 0, 3)
        q_pass(part, 0, 1)
        q_pass(part, 0, 3)

    def q_far(part):
        ones[part, 2].wait_recv()
        q_down(part, 0, 2)
        q_up(part, 0, 2)
        q_pass(part, 0, 2)

    def q_from_below(part, r):
        ups[part, 0, r].wait_recv()
        if r < 2:
            q_up(part, 3, r)
        q_pass(part, 3, r)

    def q_from_above(part, r):
        downs[part, 0, r].wait_recv()
        if r >= 2:
            q_down(part, 1, r)
        q_pass(part, 1, r)

    def q_opposite(part, *parts):
        for r in parts:
            (ups[part, 3, r] if r < 2 else downs[part, 1, r]).wait_recv()
            q_pass(part, 2, r)

    def q_here(part, off, *k):
        if off % 2 == 0:
            arrived(qa.at[0, 0], across[part, off, 0])
        else:
            arrived(qa.at[0, 0, pl.ds(0, 2)], across[part, off, k[0]])

    q_spread(0)
    q_spread(1)
    q_first(0)
    q_first(1)
    product(pairs[2])
    product(pairs[3])
    q_near(0)
    q_near(1)
    q_far(0)
    q_far(1)
    q_from_below(0, 0)
    q_from_below(1, 0)
    q_from_above(0, 0)
    q_from_above(1, 0)

    def final(part, blocks, opening=False):
        lhs, cols = ((psi_h, psi_l), slice(0, 512)) if part == 0 else ((turn_h, turn_l), slice(512, 1024))
        pieces, ks = [], []
        for target, k in blocks:
            pieces += [q[part][c, target, 2 * k + odd] for odd in range(2) for c in range(2)]
            ks.append(aligned(512 * k + 128 * target if part == 0 else 256 * target + 128 * k, 128, 128))
        rhs_h, rhs_l = split(jnp.concatenate(pieces, axis=0))
        for i in range(4):
            rows = pl.ds(256 * i, 256)
            lhs_h, lhs_l = (jnp.concatenate([ref[rows, k] for k in ks], axis=1) for ref in lhs)
            if opening:
                start = jnp.concatenate([psi_v[rows, pl.ds(256 * n + 128 * part, 128)] for n in range(4)], axis=1)
            else:
                start = acc[rows, cols]
            acc[rows, cols] = start + dot3(lhs_h, lhs_l, rhs_h, rhs_l)

    def final_whole(part, off):
        q_here(part, off)
        target = mod(first[part] + off, 4)
        final(part, [(target, 0), (target, 1)], off == 0)

    def final_beside(part, late):
        for off in (3, 1):
            q_here(part, off, late)
        k = mod(lax.div(second[part], 2) + late, 2)
        final(part, [(mod(first[part] + off, 4), k) for off in (3, 1)])

    final_whole(0, 0)
    for part in range(2):
        q_from_below(part, 1)
        q_from_above(part, 1)
    for part in range(2):
        q_from_above(part, 3)
    final_whole(1, 0)
    final_beside(0, 0)
    for part in range(2):
        q_from_above(part, 2)
        q_from_below(part, 3)
    for part in range(2):
        q_from_below(part, 2)
    final_beside(1, 0)
    final_beside(0, 1)
    for part in range(2):
        q_opposite(part, 0, 1, 3)
    arrived(zr.at[pl.ds(0, 3)], outs)
    proj_v[...] = jnp.transpose(jnp.concatenate([po[j] for j in range(4)], axis=0))
    mine = aligned(32 * (2 * z_odd + core), 32, 32)
    out = pltpu.make_async_copy(proj_v.at[mine], proj_hbm, out_sem.at[0])
    out.start()
    final_beside(1, 1)
    q_opposite(0, 2)
    q_opposite(1, 2)
    final_whole(0, 2)
    final_whole(1, 2)
    sizes = (pr.at[0, pl.ds(0, 2), pl.ds(0, 120)], zr.at[0], pr, relay, xr, yr, mg.at[0, pl.ds(0, 6)], mg.at[0], zr, zr, zr.at[pl.ds(0, 3)], yr, pb.at[0, pl.ds(0, 3)], qa)
    for i, ref in enumerate(sizes):
        wait_bytes(ref, send_sem.at[i])
    out.wait()


def body(psi, vpsi, kinetic, mixing):
    anywhere = pl.BlockSpec(memory_space=pl.ANY)
    shapes = [
        ((1024, 1024), F32), ((8, 128), F32), ((8, 128, 128), F32), ((1024, 1024), BF16), ((1024, 1024), BF16),
        ((1024, 1024), BF16), ((1024, 1024), BF16), ((1024, 1024), BF16), ((1024, 1024), BF16), ((1024, 1024), BF16), ((1024, 1024), BF16),
        ((2, 4, 2, 128, 512), F32), ((2, 4, 128, 512), F32), ((2, 2, 64, 512), F32), ((2, 2, 128, 512), F32), ((2, 4, 32, 512), F32),
        ((2, 3, 32, 512), F32), ((8, 32, 128), F32), ((7, 32, 128), F32), ((8, 32, 128), F32), ((4, 32, 128), F32),
        ((2, 8, 2, 8, 32, 128), F32), ((1024, 1024), BF16), ((1024, 1024), BF16),
        ((2, 4, 4, 32, 512), F32), ((2, 4, 4, 32, 512), F32), ((32, 1024), F32), ((128, 128), F32),
    ]
    residual, projected = pl.pallas_call(
        kernel,
        out_shape=(
            pltpu.VMEM((1024, 1024), F32),
            jax.ShapeDtypeStruct((32, 128), F32),
        ),
        in_specs=[anywhere] * 4,
        out_specs=(pl.BlockSpec(memory_space=pltpu.VMEM), anywhere),
        scratch_shapes=[pltpu.VMEM(shape, dtype) for shape, dtype in shapes]
        + [
            pltpu.SemaphoreType.DMA((8,)),
            pltpu.SemaphoreType.DMA((2,)),
            pltpu.SemaphoreType.DMA((len(FAMILIES),)),
            pltpu.SemaphoreType.DMA((SLOTS,)),
        ],
        compiler_params=pltpu.CompilerParams(
            collective_id=0, has_side_effects=True, vmem_limit_bytes=56 * 1024 * 1024
        ),
    )(psi, vpsi, kinetic.reshape(8, 128), mixing.T)
    return residual, projected.T


def solution(mesh):
    placed = (P(("grow", "gcol"), None), P(("grow", "gcol"), None), P(("grow", "gcol")), P("grow", "gcol"))
    return jax.shard_map(
        body,
        mesh=mesh,
        in_specs=placed,
        out_specs=(P(("grow", "gcol"), None), P("grow", "gcol")),
        check_vma=False,
    )
```

```python
import jax
import jax.numpy as jnp
from jax import lax
from jax.experimental import pallas as pl
from jax.experimental.pallas import tpu as pltpu
from jax.sharding import PartitionSpec as P

MESH = pl.DeviceIdType.MESH
F32, BF16 = jnp.float32, jnp.bfloat16
FAMILIES = ("spread", "far", "share", "relay", "direct", "second", "mix", "pass", "zsum", "zall", "out", "ones", "turn", "across")
SLOTS = 83


def split(value):
    high = value.astype(BF16)
    return high, (value - high.astype(F32)).astype(BF16)


def dot(a, b):
    return lax.dot_general(a, b, (((1,), (0,)), ((), ())), preferred_element_type=F32)


def dot3(a_high, a_low, b_high, b_low):
    return dot(a_high, b_high) + dot(a_high, b_low) + dot(a_low, b_high)


def mod(a, n):
    return lax.rem(a, n)


def aligned(start, size, unit):
    return pl.ds(pl.multiple_of(start, unit), size)


def kernel(
    psi_hbm, vpsi_hbm, kin_hbm, mix_hbm, acc, proj_hbm,
    psi_v, kin_v, kin_cols, psi_h, psi_l, turn_h, turn_l, pt_h, pt_l, h_h, h_l,
    pb, pr, relay, xr, own, yr, zs, zr, pg, po, mg, m_h, m_l, qa, qb, q_own, proj_v,
    load_sem, out_sem, send_sem, recv_sem,
):
    row, col = lax.axis_index("grow"), lax.axis_index("gcol")
    x, y_hi = mod(row, 4), lax.div(row, 4)
    core, z, y_lo = mod(col, 2), mod(lax.div(col, 2), 8), lax.div(col, 16)
    y = 2 * y_hi + y_lo
    other_core = 1 - core
    z_odd = mod(z, 2)

    def at(x=x, y=y, z=z, core=core):
        return (4 * lax.div(y, 2) + x, (mod(y, 2) * 8 + z) * 2 + core)

    slots = iter(range(SLOTS))

    def send(family, src, dst, to, slot=None):
        copy = pltpu.make_async_remote_copy(
            src_ref=src,
            dst_ref=dst,
            send_sem=send_sem.at[FAMILIES.index(family)],
            recv_sem=recv_sem.at[next(slots) if slot is None else slot],
            device_id=to,
            device_id_type=MESH,
        )
        copy.start()
        return copy

    def wait_bytes(ref, sem):
        pltpu.make_async_copy(ref, ref, sem).wait()

    def arrived(ref, slot):
        wait_bytes(ref, recv_sem.at[slot])

    own_mix = mg.at[core, z, y_hi, 4 * y_lo + x]
    small = [pltpu.make_async_copy(kin_hbm, kin_v, out_sem.at[0]), pltpu.make_async_copy(mix_hbm, own_mix, out_sem.at[1])]
    for copy in small:
        copy.start()
    for i in range(8):
        rows = pl.ds(128 * i, 128)
        pltpu.make_async_copy(psi_hbm.at[rows], psi_v.at[rows], load_sem.at[i]).start()
        pltpu.make_async_copy(vpsi_hbm.at[rows], acc.at[rows], load_sem.at[i]).start()

    flip_y = y + 1 - 2 * y_lo
    partner = at(core=other_core)
    plane = [at(x=mod(x + dx, 4), y=mod(y + dy, 4)) for dx in range(4) for dy in range(4) if dx + dy > 0]
    peers = [partner, at(y=flip_y, core=other_core)] + plane + [at(z=mod(z + d, 8)) for d in range(1, 8)]
    barrier = pltpu.get_barrier_semaphore()
    for peer in peers:
        pl.semaphore_signal(barrier, inc=1, device_id=peer, device_id_type=MESH)

    for copy in small:
        copy.wait()
    turned = jnp.transpose(jnp.concatenate([kin_v[...]] * 16, axis=0))
    for i in range(8):
        kin_cols[i] = jnp.broadcast_to(turned[:, i : i + 1], (128, 128))

    def prepare(i, carry):
        rows = aligned(128 * i, 128, 128)
        wait_bytes(psi_v.at[pl.ds(0, 256)], load_sem.at[i])
        kin = kin_cols[i]
        for j in range(8):
            cols = pl.ds(128 * j, 128)
            tile = psi_v[rows, cols]
            high, low = split(kin * tile + acc[rows, cols])
            h_h[rows, cols] = high
            h_l[rows, cols] = low
            high, low = split(jnp.transpose(tile))
            pt_h[cols, rows] = high
            pt_l[cols, rows] = low
        return carry

    lax.fori_loop(0, 8, prepare, 0)

    pl.semaphore_wait(barrier, len(peers))

    plane_blocks = pr.at[0, 0, pl.ds(0, 120)]
    spread = next(slots)
    for peer in plane:
        send("spread", own_mix, own_mix, peer, spread)
    across_z = mod(z + 4, 8)
    far_block = send("far", own_mix, own_mix, at(z=across_z))

    passed = [next(slots) for distance in range(5)]
    far_spread = next(slots)

    def mixing_pass(slab, half, distance):
        ref = mg.at[core, slab, half]
        send("pass", ref, ref, partner, passed[distance])

    def mixing_here(distance):
        arrived(mg.at[0, 0] if distance in (0, 4) else mg.at[0, pl.ds(0, 2)], passed[distance])

    def mixing_send(slab, half, step):
        ref = mg.at[core, slab, half]
        return send("mix", ref, ref, at(z=mod(z + step + 8, 8)))

    up, down = {}, {}

    def mixing_start():
        arrived(plane_blocks, spread)
        up[1, 0] = mixing_send(z, 0, 1)
        down[1, 0] = mixing_send(z, 1, -1)
        up[1, 1] = mixing_send(z, 1, 1)
        down[1, 1] = mixing_send(z, 0, -1)
        for half in range(2):
            mixing_pass(z, half, 0)

    def mixing_forward(distance, k):
        below, above = mod(z + 8 - distance, 8), mod(z + distance, 8)
        up[distance + 1, k] = mixing_send(below, k, 1)
        down[distance + 1, k] = mixing_send(above, 1 - k, -1)

    def mixing_step(distance, k, forward=True):
        below, above = mod(z + 8 - distance, 8), mod(z + distance, 8)
        up[distance, k].wait_recv()
        if forward:
            up[distance + 1, k] = mixing_send(below, k, 1)
        mixing_pass(below, k, distance)
        down[distance, k].wait_recv()
        if forward:
            down[distance + 1, k] = mixing_send(above, 1 - k, -1)
        mixing_pass(above, 1 - k, distance)

    def mixing_far_start():
        far_block.wait_recv()
        ref = mg.at[core, across_z, y_hi, 4 * y_lo + x]
        for peer in plane:
            send("spread", ref, ref, peer, far_spread)

    def mixing_far_pass():
        arrived(plane_blocks, far_spread)
        for half in range(2):
            mixing_pass(across_z, half, 4)

    z_pair = lax.div(z, 2)
    pairs = (z_pair, mod(z_pair + 3 + 2 * z_odd, 4), mod(z_pair + 5 - 2 * z_odd, 4), mod(z_pair + 2, 4))

    def mixing_split(pair):
        for half in range(2):
            for k in range(8):
                tile = jnp.concatenate([mg[c, 2 * pair + odd, half, k] for odd in range(2) for c in range(2)], axis=0)
                where = (pl.ds(512 * half + 128 * (k % 4), 128), aligned(256 * pair + 128 * (k // 4), 128, 128))
                high, low = split(jnp.transpose(tile))
                m_h[where] = high
                m_l[where] = low

    def product(pair):
        cols = aligned(256 * pair, 256, 256)

        def rows_of(i, carry):
            rows = aligned(512 * i, 512, 512)
            psi_v[rows, cols] = dot3(h_h[rows, :], h_l[rows, :], m_h[:, cols], m_l[:, cols])
            return carry

        lax.fori_loop(0, 2, rows_of, 0)

    first, second = (x, y), (y, x)

    def to_first(part, f):
        return at(x=f) if part == 0 else at(y=f)

    def to_second(part, s):
        return at(y=s) if part == 0 else at(x=s)

    def share(part, off):
        target = mod(first[part] + off, 4)
        pieces = []
        for half in range(2):
            for s in range(4):
                tx, ty = (target, s) if part == 0 else (s, target)
                start = 512 * lax.div(ty, 2) + 128 * tx + 64 * mod(ty, 2) + 32 * half
                pieces.append(aligned(start, 32, 32))
        lhs_h = jnp.concatenate([pt_h[p, :] for p in pieces], axis=0)
        lhs_l = jnp.concatenate([pt_l[p, :] for p in pieces], axis=0)
        for n in range(2):
            cols = pl.ds(512 * part + 256 * n, 256)
            out = dot3(lhs_h, lhs_l, h_h[:, cols], h_l[:, cols])
            pb[part, off, 0, :, pl.ds(256 * n, 256)] = out[:128]
            pb[part, off, 1, :, pl.ds(256 * n, 256)] = out[128:]
        return send("share", pb.at[part, off, other_core], pr.at[part, off], partner)

    def joined(part, off, copy):
        copy.wait_recv()
        pb[part, off, core] += pr[part, off]

    late, early = pl.ds(0, 64), pl.ds(64, 64)
    relays, direct = {}, {}

    def far(part, copy):
        joined(part, 2, copy)
        f = first[part]
        block = pb.at[part, 2, core]
        relays[part] = (
            send("relay", block.at[late], relay.at[part, 0], to_first(part, mod(f + 1, 4))),
            send("relay", block.at[early], relay.at[part, 1], to_first(part, mod(f + 3, 4))),
        )

    def near(part, off, copy):
        joined(part, off, copy)
        side, rows = (0, early) if off == 1 else (1, late)
        block = pb.at[part, off, core]
        direct[part, off] = next(slots)
        send("direct", block.at[rows], xr.at[part, side, rows], to_first(part, mod(first[part] + off, 4)), direct[part, off])

    def relayed(part, off):
        side, rows = (0, late) if off == 1 else (1, early)
        relays[part][side].wait_recv()
        pb[part, off, core, rows] += relay[part, side]
        block = pb.at[part, off, core]
        send("direct", block.at[rows], xr.at[part, side, rows], to_first(part, mod(first[part] + off, 4)), direct[part, off])

    seconds = {}

    def own_first(part):
        arrived(xr.at[part, 0], direct[part, 1])
        arrived(xr.at[part, 1], direct[part, 3])
        own[part] = (pb[part, 0, core] + xr[part, 0] + xr[part, 1]).reshape(4, 32, 512)
        s = second[part]
        seconds[part] = next(slots)
        for d in (2, 1, 3):
            to = mod(s + d, 4)
            send("second", own.at[part, to], yr.at[part, d - 1], to_second(part, to), seconds[part])

    def own_second(part):
        arrived(yr.at[part], seconds[part])
        total = own[part, second[part]] + yr[part, 0] + yr[part, 1] + yr[part, 2]
        for j in range(4):
            zs[4 * part + j] = total[:, 128 * j : 128 * (j + 1)]

    a2 = share(0, 2)
    b2 = share(1, 2)
    a1 = share(0, 1)
    far(0, a2)
    far(1, b2)
    b1 = share(1, 1)
    near(0, 1, a1)
    a3 = share(0, 3)
    near(1, 1, b1)
    mixing_start()
    b3 = share(1, 3)
    near(0, 3, a3)
    a0 = share(0, 0)
    near(1, 3, b3)
    relayed(0, 1)
    relayed(0, 3)
    relayed(1, 1)
    relayed(1, 3)
    b0 = share(1, 0)
    mixing_step(1, 0)

    def natural(i, carry):
        rows = aligned(128 * i, 128, 128)
        high, low = split(psi_v[rows, :])
        psi_h[rows, :] = high
        psi_l[rows, :] = low
        for k in range(4):
            left, right = psi_v[rows, 256 * k : 256 * k + 128], psi_v[rows, 256 * k + 128 : 256 * (k + 1)]
            for yl in range(2):
                lanes = slice(64 * yl, 64 * (yl + 1))
                high, low = split(jnp.concatenate([left[:, lanes], right[:, lanes]], axis=1))
                cols = pl.ds(512 * (k // 2) + 256 * yl + 128 * (k % 2), 128)
                turn_h[rows, cols] = high
                turn_l[rows, cols] = low
        return carry

    lax.fori_loop(0, 5, natural, 0)
    mixing_step(1, 1)
    lax.fori_loop(5, 8, natural, 0)
    joined(0, 0, a0)
    joined(1, 0, b0)
    own_first(0)
    own_first(1)
    mixing_step(2, 0)
    mixing_here(0)
    mixing_here(1)
    mixing_split(pairs[0])
    product(pairs[0])
    mixing_step(2, 1, forward=False)
    own_second(0)
    own_second(1)
    order = (4, 3, 5, 2, 6, 1, 7)
    z_sum, z_all = next(slots), next(slots)
    for d in order:
        to = mod(z + d, 8)
        send("zsum", zs.at[to], zr.at[d - 1], at(z=to), z_sum)
    mixing_forward(2, 1)
    mixing_far_start()
    mixing_here(2)
    mixing_split(pairs[1])
    mixing_step(3, 0, forward=False)
    product(pairs[1])
    arrived(zr, z_sum)
    total = zs[z]
    for d in range(7):
        total = total + zr[d]
    pg[z] = total * (1.0 / (256 * 1024))
    for d in order:
        send("zall", pg.at[z], pg.at[z], at(z=mod(z + d, 8)), z_all)
    mixing_far_pass()
    mixing_step(3, 1, forward=False)
    mixing_here(3)
    mixing_split(pairs[2])
    mixing_here(4)
    mixing_split(pairs[3])
    arrived(zr, z_all)

    block = 4 * y_lo + lax.div(z, 2)
    group = 2 * y_lo + core
    po[group] = pg[block]
    outs = next(slots)
    for dy, dc in ((0, 1), (1, 0), (1, 1)):
        to_y, to_core = (flip_y if dy else y), (other_core if dc else core)
        send("out", pg.at[4 * mod(to_y, 2) + lax.div(z, 2)], po.at[group], at(y=to_y, core=to_core), outs)

    p_h, p_l = split(jnp.concatenate([pg[j] for j in range(8)], axis=1))
    p_both = jnp.concatenate([p_h, p_l], axis=0)
    for n in range(4):
        cols = pl.ds(256 * n, 256)
        both = dot(p_both, m_h[:, cols])
        q_own[:, cols] = -(both[:32] + dot(p_h, m_l[:, cols]) + both[32:])
    for n in range(4):
        qa[core, x, y, :, pl.ds(128 * n, 128)] = q_own[:, pl.ds(256 * n, 128)]
        qb[core, y, x, :, pl.ds(128 * n, 128)] = q_own[:, pl.ds(256 * n + 128, 128)]
    q = (qa, qb)
    ones, ups, downs = {}, {}, {}
    across = {(part, off, k): next(slots) for part in range(2) for off in range(4) for k in range(1 + off % 2)}

    def piece(part, off, r):
        s = mod(second[part] + (r & 2), 4)
        return q[part].at[core, mod(first[part] + off, 4), s + 1 - 2 * mod(s, 2) if r & 1 else s]

    def q_up(part, off, r):
        ref = piece(part, off, r)
        ups[part, off, r] = send("turn", ref, ref, to_first(part, mod(first[part] + 1, 4)))

    def q_down(part, off, r):
        ref = piece(part, off, r)
        downs[part, off, r] = send("turn", ref, ref, to_first(part, mod(first[part] + 3, 4)))

    def q_pass(part, off, r):
        ref = piece(part, off, r)
        send("across", ref, ref, partner, across[part, off, (off & 1) * (r >> 1)])

    def q_spread(part):
        ref = piece(part, 0, 0)
        for d in (1, 3, 2):
            to = mod(second[part] + (d & 2), 4)
            ones[part, d] = send("ones", ref, ref, to_second(part, to + 1 - 2 * mod(to, 2) if d & 1 else to))

    def q_first(part):
        q_up(part, 0, 0)
        q_down(part, 0, 0)
        q_pass(part, 0, 0)

    def q_near(part):
        ones[part, 1].wait_recv()
        q_up(part, 0, 1)
        q_down(part, 0, 1)
        ones[part, 3].wait_recv()
        q_down(part, 0, 3)
        q_up(part, 0, 3)
        q_pass(part, 0, 1)
        q_pass(part, 0, 3)

    def q_far(part):
        ones[part, 2].wait_recv()
        q_down(part, 0, 2)
        q_up(part, 0, 2)
        q_pass(part, 0, 2)

    def q_from_below(part, r):
        ups[part, 0, r].wait_recv()
        if r < 2:
            q_up(part, 3, r)
        q_pass(part, 3, r)

    def q_from_above(part, r):
        downs[part, 0, r].wait_recv()
        if r >= 2:
            q_down(part, 1, r)
        q_pass(part, 1, r)

    def q_opposite(part, *parts):
        for r in parts:
            (ups[part, 3, r] if r < 2 else downs[part, 1, r]).wait_recv()
            q_pass(part, 2, r)

    def q_here(part, off, *k):
        if off % 2 == 0:
            arrived(qa.at[0, 0], across[part, off, 0])
        else:
            arrived(qa.at[0, 0, pl.ds(0, 2)], across[part, off, k[0]])

    q_spread(0)
    q_spread(1)
    q_first(0)
    q_first(1)
    product(pairs[2])
    product(pairs[3])
    q_near(0)
    q_near(1)
    q_far(0)
    q_far(1)
    q_from_below(0, 0)
    q_from_below(1, 0)
    q_from_above(0, 0)
    q_from_above(1, 0)

    def final(part, blocks, opening=False):
        lhs, cols = ((psi_h, psi_l), slice(0, 512)) if part == 0 else ((turn_h, turn_l), slice(512, 1024))
        pieces, ks = [], []
        for target, k in blocks:
            pieces += [q[part][c, target, 2 * k + odd] for odd in range(2) for c in range(2)]
            ks.append(aligned(512 * k + 128 * target if part == 0 else 256 * target + 128 * k, 128, 128))
        rhs_h, rhs_l = split(jnp.concatenate(pieces, axis=0))
        for i in range(4):
            rows = pl.ds(256 * i, 256)
            lhs_h, lhs_l = (jnp.concatenate([ref[rows, k] for k in ks], axis=1) for ref in lhs)
            if opening:
                start = jnp.concatenate([psi_v[rows, pl.ds(256 * n + 128 * part, 128)] for n in range(4)], axis=1)
            else:
                start = acc[rows, cols]
            acc[rows, cols] = start + dot3(lhs_h, lhs_l, rhs_h, rhs_l)

    def final_whole(part, off):
        q_here(part, off)
        target = mod(first[part] + off, 4)
        final(part, [(target, 0), (target, 1)], off == 0)

    def final_beside(part, late):
        for off in (3, 1):
            q_here(part, off, late)
        k = mod(lax.div(second[part], 2) + late, 2)
        final(part, [(mod(first[part] + off, 4), k) for off in (3, 1)])

    final_whole(0, 0)
    for part in range(2):
        q_from_below(part, 1)
        q_from_above(part, 1)
    for part in range(2):
        q_from_above(part, 3)
    final_whole(1, 0)
    final_beside(0, 0)
    for part in range(2):
        q_from_above(part, 2)
        q_from_below(part, 3)
    for part in range(2):
        q_from_below(part, 2)
    final_beside(1, 0)
    final_beside(0, 1)
    for part in range(2):
        q_opposite(part, 0, 1, 3)
    arrived(zr.at[pl.ds(0, 3)], outs)
    proj_v[...] = jnp.transpose(jnp.concatenate([po[j] for j in range(4)], axis=0))
    mine = aligned(32 * (2 * z_odd + core), 32, 32)
    out = pltpu.make_async_copy(proj_v.at[mine], proj_hbm, out_sem.at[0])
    out.start()
    final_beside(1, 1)
    q_opposite(0, 2)
    q_opposite(1, 2)
    final_whole(0, 2)
    final_whole(1, 2)
    sizes = (pr.at[0, pl.ds(0, 2), pl.ds(0, 120)], zr.at[0], pr, relay, xr, yr, mg.at[0, pl.ds(0, 6)], mg.at[0], zr, zr, zr.at[pl.ds(0, 3)], yr, pb.at[0, pl.ds(0, 3)], qa)
    for i, ref in enumerate(sizes):
        wait_bytes(ref, send_sem.at[i])
    out.wait()


def body(psi, vpsi, kinetic, mixing):
    anywhere = pl.BlockSpec(memory_space=pl.ANY)
    shapes = [
        ((1024, 1024), F32), ((8, 128), F32), ((8, 128, 128), F32), ((1024, 1024), BF16), ((1024, 1024), BF16),
        ((1024, 1024), BF16), ((1024, 1024), BF16), ((1024, 1024), BF16), ((1024, 1024), BF16), ((1024, 1024), BF16), ((1024, 1024), BF16),
        ((2, 4, 2, 128, 512), F32), ((2, 4, 128, 512), F32), ((2, 2, 64, 512), F32), ((2, 2, 128, 512), F32), ((2, 4, 32, 512), F32),
        ((2, 3, 32, 512), F32), ((8, 32, 128), F32), ((7, 32, 128), F32), ((8, 32, 128), F32), ((4, 32, 128), F32),
        ((2, 8, 2, 8, 32, 128), F32), ((1024, 1024), BF16), ((1024, 1024), BF16),
        ((2, 4, 4, 32, 512), F32), ((2, 4, 4, 32, 512), F32), ((32, 1024), F32), ((128, 128), F32),
    ]
    residual, projected = pl.pallas_call(
        kernel,
        out_shape=(
            pltpu.VMEM((1024, 1024), F32),
            jax.ShapeDtypeStruct((32, 128), F32),
        ),
        in_specs=[anywhere] * 4,
        out_specs=(pl.BlockSpec(memory_space=pltpu.VMEM), anywhere),
        scratch_shapes=[pltpu.VMEM(shape, dtype) for shape, dtype in shapes]
        + [
            pltpu.SemaphoreType.DMA((8,)),
            pltpu.SemaphoreType.DMA((2,)),
            pltpu.SemaphoreType.DMA((len(FAMILIES),)),
            pltpu.SemaphoreType.DMA((SLOTS,)),
        ],
        compiler_params=pltpu.CompilerParams(
            collective_id=0, has_side_effects=True, vmem_limit_bytes=56 * 1024 * 1024
        ),
    )(psi, vpsi, kinetic.reshape(8, 128), mixing.T)
    return residual, projected.T


def solution(mesh):
    placed = (P(("grow", "gcol"), None), P(("grow", "gcol"), None), P(("grow", "gcol")), P("grow", "gcol"))
    return jax.shard_map(
        body,
        mesh=mesh,
        in_specs=placed,
        out_specs=(P(("grow", "gcol"), None), P("grow", "gcol")),
        check_vma=False,
    )
```
